32 devices in a mesh: gx: 8 (over z, x), yz: 4 (over y, core).
Axes of the slice: x: 2, y: 2, z: 4, core: 2. Of those that a mesh axis runs over, the one named last changes fastest.
Arguments:
- state: float32 [4, 256, 192, 256], P(None, 'gx', 'yz'), may hold values from -6 to 6
- mean_flow: float32 [256, 192, 256], P('gx', 'yz'), may hold values from 0.2 to 1.2
- face_cell: int32 [6144], P(('gx', 'yz')), may hold values from 0 to 12582911, as said below
- face_normal: float32 [3, 6144], P(None, ('gx', 'yz')), may hold values from -3 to 3
- face_pos: float32 [3, 6144], P(None, ('gx', 'yz')), may hold values from -2 to 2
- observer_pos: float32 [3, 512], replicated, may hold values from 4 to 12
- time_bin: int32 [6144, 512], P(('gx', 'yz')), may hold values from 0 to 63
Outputs:
- state_next: float32 [4, 256, 192, 256], P(None, 'gx', 'yz')
- signal: float32 [512, 64], P(('gx', 'yz'))
The draws below stay inside these ranges and needn't reach their ends.
Inputs may be any that keep to these rules, and one draw needn't show every extreme that they name: `face_cell`: face j is held by device j // 192 of gx+yz, and its cell, numbered (x 192 + y) * 256 + z, lies in that device's block of grid cells.
All inputs are finite; a program needn't handle non-finite values.
Results may differ from the reference program's by a relative error of at most 0.000084.
Values sent between devices are 32-bit elements; how exact they have to be, the bound alone decides.
A program may use at most 192 MiB of HBM per device.

```python
import jax
import jax.numpy as jnp
from jax import lax

CX = 32
CY = 48
NZ = 256
FACES_DEV = 192
OBS = 512
BINS = 64
NX = 256
NY = 192
FACES = 6144
N_YZ = 4


def draw_face_cell(key, part):
    faces = jnp.arange(FACES, dtype=jnp.int32)
    device = faces // FACES_DEV
    column = device // N_YZ
    group = device % N_YZ
    key_x, key_y, key_z = jax.random.split(key, 3)
    along_x = jax.random.randint(key_x, (FACES,), 0, CX, dtype=jnp.int32)
    along_y = jax.random.randint(key_y, (FACES,), 0, CY, dtype=jnp.int32)
    along_z = jax.random.randint(key_z, (FACES,), 0, NZ, dtype=jnp.int32)
    cell = ((column * CX + along_x) * (CY * N_YZ) + group * CY + along_y) * NZ + along_z
    return cell.astype(jnp.int32)


def with_ends(entries, own_key, least, top_value):
    spot = [jax.random.randint(jax.random.fold_in(own_key, axis), (), 0, length) for axis, length in enumerate(entries.shape)]
    main_axis = entries.shape.index(max(entries.shape))
    beside = spot[:main_axis] + [(spot[main_axis] + 1) % entries.shape[main_axis]] + spot[main_axis + 1:]
    return entries.at[tuple(spot)].set(least).at[tuple(beside)].set(top_value)


def block_scale(stream_key, shape, pieces, least, high):
    loudness = 1.0
    for dim, shards_of in pieces:
        heights = jax.random.uniform(jax.random.fold_in(jax.random.fold_in(stream_key, 6), dim), (shards_of,), jnp.float32, least / len(pieces), high / len(pieces))
        loudness = loudness * jnp.repeat(jnp.exp(heights), shape[dim] // shards_of).reshape((-1,) + (1,) * (len(shape) - 1 - dim))
    return loudness


def bell_draw(own_key, extent, width, limit, shards=(), kind=jnp.bfloat16):
    factor_of = block_scale(own_key, extent, shards, -0.22, 0.18) if shards else 1.0
    array = jax.random.normal(own_key, extent, jnp.float32) * width * factor_of
    return jnp.minimum(jnp.maximum(array, -limit), limit).astype(kind)


def setup_inputs(seed: int = 0) -> dict:
    key_list = jax.random.split(jax.random.key(seed), 8)
    state = bell_draw(key_list[0], (4, NX, NY, NZ), 1.0, 6.0, ((1, 8), (2, 4)), jnp.float32)
    mean_flow = jnp.clip(0.2 + 1 * jax.random.uniform(key_list[1], (NX, NY, NZ), jnp.float32) ** block_scale(key_list[1], (NX, NY, NZ), ((0, 8), (1, 4)), -0.2, 0.2), 0.2, 1.2)
    face_cell = draw_face_cell(jax.random.fold_in(key_list[7], 71), 0)
    face_normal = jnp.clip(jax.random.uniform(key_list[3], (3, FACES), jnp.float32, -3.0, 3.0) * block_scale(key_list[3], (3, FACES), ((1, 32),), -0.4, 0.0), -3.0, 3.0)
    face_pos = jnp.clip(jax.random.uniform(key_list[4], (3, FACES), jnp.float32, -2.0, 2.0) * block_scale(key_list[4], (3, FACES), ((1, 32),), -0.4, 0.0), -2.0, 2.0)
    observer_pos = jnp.clip(jax.random.uniform(key_list[5], (3, OBS), jnp.float32, 4.0, 12.0), 4.0, 12.0)
    time_bin = with_ends(jax.random.randint(key_list[6], (FACES, OBS), 0, BINS), jax.random.fold_in(key_list[6], 1), 0, BINS - 1).astype(jnp.int32)
    return dict(state=state, mean_flow=mean_flow, face_cell=face_cell, face_normal=face_normal, face_pos=face_pos, observer_pos=observer_pos, time_bin=time_bin)


time_step = 0.25
four_pi = 4.0 * 3.141592653589793

def diagonals(count, dtype):
    index = jnp.arange(count)
    third = jnp.full((count,), 1.0 / 3.0, dtype)
    quarter = jnp.asarray(0.25, dtype)
    lower = jnp.where(index == 1, quarter, third)
    lower = jnp.where(index == count - 2, quarter, lower)
    lower = jnp.where(index == count - 1, jnp.asarray(2.0, dtype), lower)
    lower = jnp.where(index == 0, jnp.asarray(0.0, dtype), lower)
    upper = jnp.where(index == 1, quarter, third)
    upper = jnp.where(index == count - 2, quarter, upper)
    upper = jnp.where(index == 0, jnp.asarray(2.0, dtype), upper)
    upper = jnp.where(index == count - 1, jnp.asarray(0.0, dtype), upper)
    return (lower, jnp.ones((count,), dtype), upper)

def compact_rhs(field, axis):
    count = field.shape[axis]
    widths = [(2, 2) if dimension == axis else (0, 0) for dimension in range(field.ndim)]
    padded = jnp.pad(field, widths)

    def take(first, last):
        return lax.slice_in_dim(padded, first, last, axis=axis)

    def plane(index):
        return lax.slice_in_dim(field, index, index + 1, axis=axis)
    inner = 7.0 / 9.0 * (take(3, count + 3) - take(1, count + 1)) + 1.0 / 36.0 * (take(4, count + 4) - take(0, count))
    first_row = 0.5 * (4.0 * plane(1) + plane(2) - 5.0 * plane(0))
    second_row = 0.75 * (plane(2) - plane(0))
    before_last = 0.75 * (plane(count - 1) - plane(count - 3))
    last_row = 0.5 * (5.0 * plane(count - 1) - 4.0 * plane(count - 2) - plane(count - 3))
    middle_rows = lax.slice_in_dim(inner, 2, count - 2, axis=axis)
    return jnp.concatenate([first_row, second_row, middle_rows, before_last, last_row], axis)

def compact_derivative(field, axis):
    moved = jnp.moveaxis(compact_rhs(field, axis), axis, 0)
    count = moved.shape[0]
    lower, middle, upper = diagonals(count, field.dtype)
    solved = lax.linalg.tridiagonal_solve(lower, middle, upper, moved.reshape(count, -1))
    return jnp.moveaxis(solved.reshape(moved.shape), 0, axis)

def explicit_y(field):
    count = field.shape[1]
    padded = jnp.pad(field, ((0, 0), (3, 3), (0, 0)))

    def take(shift):
        return padded[:, 3 + shift:3 + shift + count]
    return 0.75 * (take(1) - take(-1)) - 0.15 * (take(2) - take(-2)) + 1.0 / 60.0 * (take(3) - take(-3))

def reference(state, mean_flow, face_cell, face_normal, face_pos, observer_pos, time_bin):
    pressure, stream, lateral, vertical = (state[0], state[1], state[2], state[3])
    pressure_x = compact_derivative(pressure, 0)
    stream_x = compact_derivative(stream, 0)
    lateral_x = compact_derivative(lateral, 0)
    vertical_x = compact_derivative(vertical, 0)
    mean_x = compact_derivative(mean_flow, 0)
    pressure_y = explicit_y(pressure)
    lateral_y = explicit_y(lateral)
    mean_y = explicit_y(mean_flow)
    pressure_z = compact_derivative(pressure, 2)
    vertical_z = compact_derivative(vertical, 2)
    mean_z = compact_derivative(mean_flow, 2)
    pressure_rate = -(mean_flow * pressure_x + stream_x + lateral_y + vertical_z)
    stream_rate = -(mean_flow * stream_x + stream * mean_x + lateral * mean_y + vertical * mean_z + pressure_x)
    lateral_rate = -(mean_flow * lateral_x + pressure_y)
    vertical_rate = -(mean_flow * vertical_x + pressure_z)
    rates = jnp.stack([pressure_rate, stream_rate, lateral_rate, vertical_rate])
    state_next = state + time_step * rates
    face_rates = rates.reshape(4, -1)[:, face_cell]
    face_pressure = state_next[0].reshape(-1)[face_cell]
    normal_rate = face_normal[0] * face_rates[1] + face_normal[1] * face_rates[2] + face_normal[2] * face_rates[3]
    offset_x = observer_pos[0][None, :] - face_pos[0][:, None]
    offset_y = observer_pos[1][None, :] - face_pos[1][:, None]
    offset_z = observer_pos[2][None, :] - face_pos[2][:, None]
    distance = jnp.sqrt(offset_x * offset_x + offset_y * offset_y + offset_z * offset_z)
    normal_r = (face_normal[0][:, None] * offset_x + face_normal[1][:, None] * offset_y + face_normal[2][:, None] * offset_z) / distance
    contribution = (normal_rate[:, None] + (face_rates[0][:, None] + face_pressure[:, None] / distance) * normal_r) / (four_pi * distance)
    slots = jnp.arange(OBS, dtype=jnp.int32)[None, :] * BINS + time_bin
    signal = jnp.zeros((OBS * BINS,), contribution.dtype).at[slots.reshape(-1)].add(contribution.reshape(-1))
    return (state_next, signal.reshape(OBS, BINS))
```

```python
import functools

import numpy as np
import jax
import jax.numpy as jnp
from jax import lax
from jax.experimental import pallas as pl
from jax.experimental.pallas import tpu as pltpu
from jax.sharding import PartitionSpec as P

BINS = 64
TILE = 8
LANES = 128
REACH = 3
VMEM_MIB = 54

time_step = 0.25
four_pi = 4.0 * 3.141592653589793
VMEM = pltpu.VMEM
SMEM = pltpu.SMEM
HBM = pltpu.HBM
MESH = pl.DeviceIdType.MESH

PADDED = (0, 2, 4)
PLAIN = (1, 3)


def diagonals(count):
    lower = np.full(count, 1.0 / 3.0)
    upper = np.full(count, 1.0 / 3.0)
    lower[1] = lower[count - 2] = upper[1] = upper[count - 2] = 0.25
    lower[0] = upper[count - 1] = 0.0
    lower[count - 1] = upper[0] = 2.0
    return lower, upper


def stencil(count):
    rows = np.zeros((count, count))
    for i in range(2, count - 2):
        rows[i, i + 1], rows[i, i - 1] = 7.0 / 9.0, -7.0 / 9.0
        rows[i, i + 2], rows[i, i - 2] = 1.0 / 36.0, -1.0 / 36.0
    rows[0, :3] = (-2.5, 2.0, 0.5)
    rows[1, 0], rows[1, 2] = -0.75, 0.75
    rows[count - 2, count - 3], rows[count - 2, count - 1] = -0.75, 0.75
    rows[count - 1, count - 3:] = (-0.5, -2.0, 2.5)
    return rows


def dense_derivative(count):
    lower, upper = diagonals(count)
    matrix = np.eye(count) + np.diag(lower[1:], -1) + np.diag(upper[:-1], 1)
    return np.linalg.solve(matrix, stencil(count))


class Table:
    def __init__(self, blocks, cells):
        count = blocks * cells
        lower, upper = diagonals(count)
        rows = stencil(count)
        down, pivot = np.zeros(count), np.ones(count)
        for i in range(1, count):
            down[i] = lower[i] / pivot[i - 1]
            pivot[i] = 1.0 - down[i] * upper[i - 1]
        up, pivot_up = np.zeros(count), np.ones(count)
        for i in range(count - 2, -1, -1):
            up[i] = upper[i] / pivot_up[i + 1]
            pivot_up[i] = 1.0 - up[i] * lower[i + 1]
        from_left = rows.copy()
        for i in range(1, count):
            from_left[i] -= down[i] * from_left[i - 1]
        from_right = rows.copy()
        for i in range(count - 2, -1, -1):
            from_right[i] -= up[i] * from_right[i + 1]
        part = {
            "right": np.zeros((blocks, cells)), "left": np.zeros((blocks, cells)),
            "near": np.zeros((blocks, cells)), "wide": np.zeros((blocks, cells)),
            "back": np.zeros((blocks, cells)), "ahead": np.zeros((blocks, cells)),
            "edge": np.zeros((blocks, 4, 4)), "link": np.zeros((blocks, 4)),
            "ends": np.zeros((blocks, 4)),
        }
        chain = np.zeros((blocks, 2))
        for d in range(blocks):
            s, e = d * cells, (d + 1) * cells
            if d < blocks - 1:
                part["right"][d] = from_left[e + 1, s:e]
                chain[d, 0] = np.prod(-down[s + 2:e + 2])
            if d > 0:
                part["left"][d] = from_right[s - 2, s:e]
                chain[d, 1] = np.prod(-up[s - 2:e - 2])
            inverse = 1.0 / pivot[s:e]
            inverse[-1] = 1.0 / (pivot[e - 1] + pivot_up[e - 1] - 1.0)
            part["near"][d] = 7.0 / 9.0 * inverse
            part["wide"][d] = 1.0 / 36.0 * inverse
            part["back"][d] = lower[s:e] * inverse
            part["ahead"][d] = upper[s:e] / pivot[s:e]
            part["edge"][d, 0, :3] = from_left[s, s:s + 3] * inverse[0]
            part["edge"][d, 1] = rows[s + 1, s:s + 4] * inverse[1]
            part["edge"][d, 2] = rows[e - 2, e - 4:e] * inverse[-2]
            part["edge"][d, 3, 1:] = from_right[e - 1, e - 3:e] * inverse[-1]
            part["ends"][d, 0] = -inverse[0] / down[s + 1]
            part["ends"][d, 1] = -inverse[-1] / up[e - 2]
            if d > 0:
                part["ends"][d, 2] = rows[s + 1, s - 1] / lower[s + 1]
            if d < blocks - 1:
                part["ends"][d, 3] = rows[e - 2, e] / upper[e - 2]
        part["link"][1:, 0] = chain[1:, 0] * chain[:-1, 0]
        part["link"][:-1, 1] = chain[:-1, 1] * chain[1:, 1]
        part["link"][1:, 2] = chain[:-1, 0]
        part["link"][:-1, 3] = chain[1:, 1]
        largest, hops, reach = np.abs(chain).max(), 1, np.abs(chain).max()
        while hops < blocks - 1 and reach >= np.finfo(np.float32).tiny:
            hops, reach = hops + 1, reach * largest
        assert hops <= 3
        self.at, column = {}, 0
        for name, values in part.items():
            self.at[name] = column
            column += values[0].size
        self.stride = column
        self.values = np.concatenate(
            [values.reshape(blocks, -1) for values in part.values()], axis=1
        ).astype(np.float32).reshape(-1)


def quotient(largest, divisor):
    for shift in range(31):
        factor = -(-(1 << shift) // divisor)
        excess = factor * divisor - (1 << shift)
        if excess * (largest - 1) < (1 << shift) and factor * (largest - 1) < 2**31:
            return factor, shift
    raise AssertionError("no factor")


def fused_kernel(
    sizes, where, stride,
    table_ref, cell_ref, state_ref, flow_ref, zhi_in, zlo_in,
    cells_ref, normal_ref, pos_ref, observer_ref, bin_in,
    next_ref, signal_ref,
    zhi_ref, zlo_ref, bin_ref, pad, plain, base, swept, rate,
    to_right, to_left, left_sum, right_sum, on_right, on_left, far_left, far_right,
    left_plane, right_plane,
    geometry, kernels, picked, contribution, binned, pieces, landing,
    load_sem, halo_send, halo_recv, plane_send, plane_recv, sum_send, sum_recv,
    piece_send, piece_recv,
):
    blocks, groups = sizes
    _, cells, width, depth = next_ref.shape
    faces, observers = bin_ref.shape
    tiles, halves, count = width // TILE, depth // LANES, blocks * groups
    block, group = lax.axis_index("gx"), lax.axis_index("yz")
    me = block * groups + group
    row0 = block * stride

    def scalar(name, i=0):
        return table_ref[row0 + (where[name] + i)]

    place = {"gx": (block, blocks), "yz": (group, groups)}

    def there(axis, shift):
        index, number = place[axis]
        return index + shift < number if shift > 0 else index + shift >= 0

    def other(axis, shift):
        index, number = place[axis]
        return {axis: jnp.clip(index + shift, 0, number - 1)}

    def partner(k):
        index = lax.rem(me + k, count)
        return {"gx": lax.div(index, groups), "yz": lax.rem(index, groups)}, index

    barrier = pltpu.get_barrier_semaphore()
    for k in range(1, count):
        pl.semaphore_signal(barrier, inc=1, device_id=partner(k)[0], device_id_type=MESH)

    loads = []
    for slot, f in enumerate(PADDED):
        source = flow_ref if f == 4 else state_ref.at[f]
        for h in range(halves):
            loads.append(pltpu.make_async_copy(
                source.at[:, :, h * LANES:(h + 1) * LANES],
                pad.at[slot, h, :, TILE:TILE + width, :], load_sem.at[len(loads)],
            ))
    for slot, f in enumerate(PLAIN):
        loads.append(pltpu.make_async_copy(state_ref.at[f], plain.at[slot], load_sem.at[len(loads)]))
    spare = [
        pltpu.make_async_copy(source, target, load_sem.at[len(loads) + k])
        for k, (source, target) in enumerate(((zhi_in, zhi_ref), (zlo_in, zlo_ref), (bin_in, bin_ref)))
    ]
    for load in loads + spare:
        load.start()

    for axis, shift, targets in (
        ("gx", -1, (left_sum, left_plane)), ("gx", 1, (right_sum, right_plane)),
        ("gx", -2, (far_left,)), ("gx", 2, (far_right,)),
    ):
        @pl.when(jnp.logical_not(there(axis, shift)))
        def _():
            for target in targets:
                target[...] = jnp.zeros_like(target)
    for shift, at in ((-1, TILE - REACH), (1, TILE + width)):
        @pl.when(jnp.logical_not(there("yz", shift)))
        def _():
            pad[:, :, :, at:at + REACH, :] = jnp.zeros((len(PADDED), halves, cells, REACH, LANES), jnp.float32)

    def remote(source, target, send, recv, axis, shift):
        return pltpu.make_async_remote_copy(
            src_ref=source, dst_ref=target, send_sem=send, recv_sem=recv,
            device_id=other(axis, shift), device_id_type=MESH,
        )

    def start(copy, axis, shift):
        @pl.when(there(axis, shift))
        def _():
            copy.start()

    def arrive(copy, axis, shift):
        @pl.when(there(axis, -shift))
        def _():
            copy.wait_recv()

    def sent(copy, axis, shift):
        @pl.when(there(axis, shift))
        def _():
            copy.wait_send()

    def near(side, t):
        if side == 0:
            return remote(on_right.at[t], left_sum.at[t], sum_send.at[0, t], sum_recv.at[0, t], "gx", 1), "gx", 1
        return remote(on_left.at[t], right_sum.at[t], sum_send.at[1, t], sum_recv.at[1, t], "gx", -1), "gx", -1

    def far(side, t):
        if side == 0:
            return remote(to_right.at[t], far_left.at[t], sum_send.at[2, t], sum_recv.at[2, t], "gx", 2), "gx", 2
        return remote(to_left.at[t], far_right.at[t], sum_send.at[3, t], sum_recv.at[3, t], "gx", -2), "gx", -2

    halos = [
        (remote(pad.at[:, :, :, TILE + width - REACH:TILE + width, :], pad.at[:, :, :, TILE - REACH:TILE, :],
                halo_send.at[0], halo_recv.at[0], "yz", 1), "yz", 1),
        (remote(pad.at[:, :, :, TILE:TILE + REACH, :], pad.at[:, :, :, TILE + width:TILE + width + REACH, :],
                halo_send.at[1], halo_recv.at[1], "yz", -1), "yz", -1),
    ]
    planes = [[], []]
    for side, (at, target, shift) in enumerate(((cells - 1, left_plane, 1), (0, right_plane, -1))):
        for piece, (source, into) in enumerate((
            (state_ref.at[0:2, at], target.at[0:2]), (state_ref.at[2:4, at], target.at[2:4]),
            (flow_ref.at[at], target.at[4]),
        )):
            planes[min(piece, 1)].append((remote(
                source, into, plane_send.at[side, piece], plane_recv.at[side, piece], "gx", shift
            ), "gx", shift))

    def value(f, i, rows, h):
        if f in PADDED:
            return pad[PADDED.index(f), h, i, pl.ds(rows + TILE, TILE), :]
        return plain[PLAIN.index(f), i, pl.ds(rows, TILE), h * LANES:(h + 1) * LANES]

    def first_row(t):
        return pl.multiple_of(t * TILE, TILE)

    pl.semaphore_wait(barrier, count - 1)
    for entry in planes[0]:
        start(*entry)
    for load in loads[:len(PADDED) * halves]:
        load.wait()
    for entry in halos:
        start(*entry)
    for load in loads[len(PADDED) * halves:] + spare:
        load.wait()

    fields = range(5)
    pairs = [(f, h) for f in fields for h in range(halves)]

    def sums(t, carry):
        rows = first_row(t)
        totals = None
        for i in range(cells):
            weights = scalar("right", i), scalar("left", i)
            now = [value(f, i, rows, h) for f, h in pairs]
            terms = [[weight * one for weight in weights] for one in now]
            totals = terms if totals is None else [
                [old + new for old, new in zip(*both)] for both in zip(totals, terms)
            ]
        for (f, h), (total_right, total_left) in zip(pairs, totals):
            lanes = slice(h * LANES, (h + 1) * LANES)
            to_right[t, f, :, lanes] = total_right
            to_left[t, f, :, lanes] = total_left
        start(*far(0, t))
        start(*far(1, t))
        return carry

    lax.fori_loop(0, tiles, sums, 0)

    together = 4 if cells % 4 == 0 else 1

    def multiply(k, carry):
        span = pl.ds(k * together, together)
        for f, target in ((0, 3), (3, 0), (4, 1)):
            if f in PADDED:
                lines = jnp.concatenate([
                    pad[PADDED.index(f), h, span, TILE:TILE + width, :].reshape(together * width, LANES)
                    for h in range(halves)
                ], axis=1)
            else:
                lines = plain[PLAIN.index(f), span].reshape(together * width, depth)
            high = lines.astype(jnp.bfloat16)
            rest = (lines - high.astype(jnp.float32)).astype(jnp.bfloat16)
            out = jnp.dot(rest, zhi_ref[...], preferred_element_type=jnp.float32)
            out += jnp.dot(high, zlo_ref[...], preferred_element_type=jnp.float32)
            out += jnp.dot(high, zhi_ref[...], preferred_element_type=jnp.float32)
            base[target, span] = out.reshape(together, width, depth)
        return carry

    lax.fori_loop(0, cells // together, multiply, 0)

    geometry[...] = jnp.zeros_like(geometry)
    geometry[0:3, 0:faces] = normal_ref[...]
    geometry[3:6, 0:faces] = pos_ref[...]
    along_z = cells_ref[...] & (depth - 1) if depth & (depth - 1) == 0 else lax.rem(cells_ref[...], depth)
    geometry[6:7, 0:faces] = along_z.astype(jnp.float32)
    columns = geometry[...].T

    def column(c):
        return columns[0:faces, c:c + 1]

    normal = [column(c) for c in range(3)]
    offset = [observer_ref[c:c + 1, :] - column(3 + c) for c in range(3)]
    distance = jnp.sqrt(offset[0] * offset[0] + offset[1] * offset[1] + offset[2] * offset[2])
    normal_r = (normal[0] * offset[0] + normal[1] * offset[1] + normal[2] * offset[2]) / distance
    scale = 1.0 / (four_pi * distance)
    kernels[0] = scale
    kernels[1] = normal_r * scale
    kernels[2] = normal_r * scale / distance

    def relay(t):
        arrive(*far(0, t))
        arrive(*far(1, t))
        on_right[t] = to_right[t] + scalar("link", 0) * far_left[t]
        on_left[t] = to_left[t] + scalar("link", 1) * far_right[t]
        start(*near(0, t))
        start(*near(1, t))

    for entry in halos:
        arrive(*entry)

    def lateral(i, carry):
        for t in range(tiles):
            rows = t * TILE
            for h in range(halves):
                lanes = slice(h * LANES, (h + 1) * LANES)

                def y_rate(slot):
                    def take(shift):
                        return pad[slot, h, i, TILE + rows + shift:2 * TILE + rows + shift, :]
                    return (
                        0.75 * (take(1) - take(-1)) - 0.15 * (take(2) - take(-2))
                        + 1.0 / 60.0 * (take(3) - take(-3))
                    )

                spot = (i, slice(rows, rows + TILE), lanes)
                base[(0,) + spot] = base[(0,) + spot] + y_rate(1)
                base[(1,) + spot] = value(2, i, rows, h) * y_rate(2) + value(3, i, rows, h) * base[(1,) + spot]
                base[(2,) + spot] = y_rate(0)
        return carry

    pumps = min(tiles, cells)
    for t in range(pumps):
        relay(t)
        lax.fori_loop(cells * t // pumps, cells * (t + 1) // pumps, lateral, 0)
    for entry in planes[1]:
        start(*entry)

    chunk = 4
    assert cells % chunk == 0 and cells >= 3 * chunk

    def finish(t):
        arrive(*near(0, t))
        arrive(*near(1, t))
        rows = first_row(t)
        n = cells
        carry = []
        edge = [scalar("edge", j) for j in range(8)]
        link, end, back = scalar("link", 2), scalar("ends", 0), scalar("back", 1)
        for f, h in pairs:
            lanes = slice(h * LANES, (h + 1) * LANES)
            own = [value(f, i, rows, h) for i in range(4)]
            incoming = left_sum[t, f, :, lanes] + link * far_left[t, f, :, lanes]
            first = edge[0] * own[0] + edge[1] * own[1] + edge[2] * own[2] + end * incoming
            second = edge[4] * own[0] + edge[5] * own[1] + edge[6] * own[2] + edge[7] * own[3] - back * first
            swept[f, 0, :, lanes] = first
            swept[f, 1, :, lanes] = second
            carry.append(second)

        def forward(k, carry):
            i0 = 2 + k * chunk
            new = list(carry)
            factors = [[scalar(name, i0 + j) for name in ("near", "wide", "back")] for j in range(chunk)]
            for p, (f, h) in enumerate(pairs):
                lanes = slice(h * LANES, (h + 1) * LANES)
                own = [value(f, i0 + j, rows, h) for j in range(-2, chunk + 2)]
                for j in range(chunk):
                    close, wide, back = factors[j]
                    new[p] = close * (own[j + 3] - own[j + 1]) + wide * (own[j + 4] - own[j]) - back * new[p]
                    swept[f, i0 + j, :, lanes] = new[p]
            return tuple(new)

        carry = lax.fori_loop(0, (n - 4) // chunk, forward, tuple(carry))
        solved = []
        edge = [scalar("edge", 8 + j) for j in range(8)]
        link, end, back, last = scalar("link", 3), scalar("ends", 1), scalar("back", n - 2), scalar("back", n - 1)
        for p, (f, h) in enumerate(pairs):
            lanes = slice(h * LANES, (h + 1) * LANES)
            own = [value(f, i, rows, h) for i in range(n - 4, n)]
            incoming = right_sum[t, f, :, lanes] + link * far_right[t, f, :, lanes]
            before = (
                edge[0] * own[0] + edge[1] * own[1] + edge[2] * own[2] + edge[3] * own[3] - back * carry[p]
            )
            swept[f, n - 2, :, lanes] = before
            solved.append(
                edge[5] * own[1] + edge[6] * own[2] + edge[7] * own[3] + end * incoming - last * before
            )

        def store(i, x):
            spot = pl.ds(pl.multiple_of(i * width + rows, TILE), TILE)
            for h in range(halves):
                lanes = slice(h * LANES, (h + 1) * LANES)
                old = [value(f, i, rows, h) for f in fields]
                flow = old[4]
                px, ux, vx, wx, fx = (x[f * halves + h] for f in fields)
                terms = [base[c, i, pl.ds(rows, TILE), lanes] for c in range(4)]
                losses = (
                    flow * px + ux + terms[0],
                    flow * ux + old[1] * fx + px + terms[1],
                    flow * vx + terms[2],
                    flow * wx + terms[3],
                )
                for c in range(4):
                    rate[c, spot, lanes] = losses[c]
                    next_ref[c, i, pl.ds(rows, TILE), lanes] = old[c] - time_step * losses[c]

        def step_back(i, x):
            ahead = scalar("ahead", i)
            x = [
                swept[f, i, :, h * LANES:(h + 1) * LANES] - ahead * x[p]
                for p, (f, h) in enumerate(pairs)
            ]
            store(i, x)
            return x

        store(n - 1, solved)
        for j in range(2, chunk + 1):
            solved = step_back(n - j, solved)

        def backward(k, x):
            for j in range(chunk):
                x = step_back(n - chunk - 1 - k * chunk - j, x)
            return tuple(x)

        lax.fori_loop(0, n // chunk - 1, backward, tuple(solved))

    def main(t, carry):
        finish(t)
        return carry

    lax.fori_loop(0, tiles, main, 0)

    for entry in planes[0] + planes[1]:
        arrive(*entry)

    def mend(t, carry):
        rows = first_row(t)
        for at, plane, end in ((0, left_plane, 2), (cells - 1, right_plane, 3)):
            spot = pl.ds(pl.multiple_of(at * width + rows, TILE), TILE)
            for h in range(halves):
                lanes = slice(h * LANES, (h + 1) * LANES)
                px, ux, vx, wx, fx = (scalar("ends", end) * plane[f, pl.ds(rows, TILE), lanes] for f in fields)
                stream, flow = value(1, at, rows, h), value(4, at, rows, h)
                more = (flow * px + ux, flow * ux + stream * fx + px, flow * vx, flow * wx)
                for c in range(4):
                    rate[c, spot, lanes] = rate[c, spot, lanes] + more[c]
                    next_ref[c, at, pl.ds(rows, TILE), lanes] = (
                        next_ref[c, at, pl.ds(rows, TILE), lanes] - time_step * more[c]
                    )
        return carry

    lax.fori_loop(0, tiles, mend, 0)

    factor, shift = quotient(cells * width * groups, width * groups)
    power = depth.bit_length() - 1
    origin = block * (cells * width * groups)

    def pick(k, carry):
        cell = cell_ref[k]
        line = (cell >> power if depth & (depth - 1) == 0 else lax.div(cell, depth)) - origin
        along_x = (line * factor) >> shift
        along_y = jnp.clip(line - along_x * (width * groups) - group * width, 0, width - 1)
        along_x = jnp.clip(along_x, 0, cells - 1)
        row = along_x * width + along_y
        for c in range(4):
            picked[c, pl.ds(k, 1), :] = rate[c, pl.ds(row, 1), :]
        picked[4, pl.ds(k, 1), :] = next_ref[0, along_x, pl.ds(along_y, 1), :]
        return carry

    lax.fori_loop(0, faces, pick, 0, unroll=4)
    mask = lax.broadcasted_iota(jnp.int32, (faces, depth), 1) == column(6).astype(jnp.int32)
    at = [jnp.sum(jnp.where(mask, picked[c], 0.0), axis=1, keepdims=True) for c in range(5)]
    normal_rate = normal[0] * at[1] + normal[1] * at[2] + normal[2] * at[3]
    contribution[...] = at[4] * kernels[2] - at[0] * kernels[1] - normal_rate * kernels[0]

    def gather(b, carry):
        binned[pl.ds(b, 1), :] = jnp.sum(
            jnp.where(bin_ref[...] == b, contribution[...], 0.0), axis=0, keepdims=True
        )
        return carry

    lax.fori_loop(0, BINS, gather, 0, unroll=2)
    share, beside = observers // count, LANES // BINS
    dense = share % (TILE * beside) == 0
    if not dense:
        pieces[...] = jnp.zeros_like(pieces)
    turned = jnp.concatenate([binned[...], jnp.zeros((LANES - BINS, observers), jnp.float32)], axis=0).T
    if dense:
        turned = turned.reshape(count, share // TILE, TILE, LANES)
        lane = lax.broadcasted_iota(jnp.int32, (count * TILE, LANES), 1)
        for q in range(share // TILE // beside):
            row = turned[:, q * beside].reshape(count * TILE, LANES)
            for j in range(1, beside):
                moved = pltpu.roll(turned[:, q * beside + j].reshape(count * TILE, LANES), j * BINS, 1)
                row = jnp.where(lane >= j * BINS, moved, row)
            pieces[:, q] = row.reshape(count, TILE, LANES)
    else:
        for d in range(count):
            pieces[d, 0, 0:share, :] = turned[d * share:(d + 1) * share]
    copies = []
    for k in range(1, count):
        target, index = partner(k)
        copies.append(pltpu.make_async_remote_copy(
            src_ref=pieces.at[index], dst_ref=landing.at[k - 1],
            send_sem=piece_send.at[k - 1], recv_sem=piece_recv.at[k - 1],
            device_id=target, device_id_type=MESH,
        ))
        copies[-1].start()
    total = pieces[me]
    for k in range(count - 1):
        copies[k].wait_recv()
        total += landing[k]
    if dense:
        for q in range(share // TILE // beside):
            for j in range(beside):
                moved = total[q] if j == 0 else pltpu.roll(total[q], LANES - j * BINS, 1)
                top = (q * beside + j) * TILE
                signal_ref[top:top + TILE, :] = moved[:, 0:BINS]
    else:
        signal_ref[...] = total[0, 0:share, 0:BINS]

    for k in range(count - 1):
        copies[k].wait_send()
    for entry in halos + planes[0] + planes[1]:
        sent(*entry)

    def drain(t, carry):
        for side in (0, 1):
            sent(*near(side, t))
            sent(*far(side, t))
        return carry

    lax.fori_loop(0, tiles, drain, 0)


def copy_kernel(next_ref, signal_ref, next_out, signal_out, sems):
    copies = [
        pltpu.make_async_copy(next_ref, next_out, sems.at[0]),
        pltpu.make_async_copy(signal_ref, signal_out, sems.at[1]),
    ]
    for copy in copies:
        copy.start()
    for copy in copies:
        copy.wait()


def per_device(sizes, state, mean_flow, face_cell, face_normal, face_pos, observer_pos, time_bin):
    blocks, groups = sizes
    _, cells, width, depth = state.shape
    faces, observers = time_bin.shape
    tiles, halves, devices = width // TILE, depth // LANES, blocks * groups
    share = observers // devices
    dense = share % (TILE * (LANES // BINS)) == 0
    packed = (share * BINS // (TILE * LANES), TILE, LANES) if dense else (1, -(-share // TILE) * TILE, LANES)
    table = Table(blocks, cells)
    operator = dense_derivative(depth).T.astype(np.float32)
    z_high = jnp.asarray(operator).astype(jnp.bfloat16)
    z_low = (jnp.asarray(operator) - z_high.astype(jnp.float32)).astype(jnp.bfloat16)
    f32 = jnp.float32
    padded_faces = -(-faces // LANES) * LANES
    smem, vmem, hbm = (pl.BlockSpec(memory_space=space) for space in (SMEM, VMEM, HBM))
    dma = pltpu.SemaphoreType.DMA
    sums = VMEM((tiles, 5, TILE, depth), f32)
    state_next, signal = pl.pallas_call(
        functools.partial(fused_kernel, sizes, table.at, table.stride),
        out_shape=(VMEM(state.shape, f32), VMEM((share, BINS), f32)),
        in_specs=[smem, smem, hbm, hbm, hbm, hbm, vmem, vmem, vmem, vmem, hbm],
        out_specs=(vmem, vmem),
        scratch_shapes=[
            VMEM((depth, depth), jnp.bfloat16), VMEM((depth, depth), jnp.bfloat16),
            VMEM((faces, observers), jnp.int32),
            VMEM((len(PADDED), halves, cells, width + 2 * TILE, LANES), f32),
            VMEM((len(PLAIN), cells, width, depth), f32),
            VMEM((4, cells, width, depth), f32),
            VMEM((5, cells, TILE, depth), f32),
            VMEM((4, cells * width, depth), f32),
        ] + [sums] * 8 + [
            VMEM((5, width, depth), f32), VMEM((5, width, depth), f32),
            VMEM((TILE, padded_faces), f32), VMEM((3, faces, observers), f32),
            VMEM((5, faces, depth), f32), VMEM((faces, observers), f32),
            VMEM((BINS, observers), f32), VMEM((devices,) + packed, f32),
            VMEM((devices - 1,) + packed, f32),
            dma((len(PADDED) * halves + len(PLAIN) + 3,)), dma((2,)), dma((2,)), dma((2, 3)), dma((2, 3)),
            dma((4, tiles)), dma((4, tiles)), dma((devices - 1,)), dma((devices - 1,)),
        ],
        compiler_params=pltpu.CompilerParams(
            collective_id=0, has_side_effects=True, vmem_limit_bytes=VMEM_MIB * 1024 * 1024
        ),
    )(
        jnp.asarray(table.values), face_cell, state, mean_flow, z_high, z_low,
        face_cell.reshape(1, faces), face_normal, face_pos, observer_pos, time_bin,
    )
    return pl.pallas_call(
        copy_kernel,
        out_shape=(
            jax.ShapeDtypeStruct(state.shape, f32),
            jax.ShapeDtypeStruct((share, BINS), f32),
        ),
        in_specs=[vmem, vmem],
        out_specs=(hbm, hbm),
        scratch_shapes=[dma((2,))],
        compiler_params=pltpu.CompilerParams(vmem_limit_bytes=8 * 1024 * 1024),
    )(state_next, signal)


def solution(mesh):
    in_specs = (
        P(None, "gx", "yz", None),
        P("gx", "yz", None),
        P(("gx", "yz")),
        P(None, ("gx", "yz")),
        P(None, ("gx", "yz")),
        P(),
        P(("gx", "yz"), None),
    )
    out_specs = (P(None, "gx", "yz", None), P(("gx", "yz"), None))
    sizes = (mesh.shape["gx"], mesh.shape["yz"])
    return jax.shard_map(
        functools.partial(per_device, sizes),
        mesh=mesh, in_specs=in_specs, out_specs=out_specs, check_vma=False,
    )
```

```python
import functools

import numpy as np
import jax
import jax.numpy as jnp
from jax import lax
from jax.experimental import pallas as pl
from jax.experimental.pallas import tpu as pltpu
from jax.sharding import PartitionSpec as P

BINS = 64
TILE = 8
LANES = 128
REACH = 3
VMEM_MIB = 54
EARLY = ()

time_step = 0.25
four_pi = 4.0 * 3.141592653589793
VMEM = pltpu.VMEM
SMEM = pltpu.SMEM
HBM = pltpu.HBM
MESH = pl.DeviceIdType.MESH

PADDED = (0, 2, 4)
PLAIN = (1, 3)


def diagonals(count):
    lower = np.full(count, 1.0 / 3.0)
    upper = np.full(count, 1.0 / 3.0)
    lower[1] = lower[count - 2] = upper[1] = upper[count - 2] = 0.25
    lower[0] = upper[count - 1] = 0.0
    lower[count - 1] = upper[0] = 2.0
    return lower, upper


def stencil(count):
    rows = np.zeros((count, count))
    for i in range(2, count - 2):
        rows[i, i + 1], rows[i, i - 1] = 7.0 / 9.0, -7.0 / 9.0
        rows[i, i + 2], rows[i, i - 2] = 1.0 / 36.0, -1.0 / 36.0
    rows[0, :3] = (-2.5, 2.0, 0.5)
    rows[1, 0], rows[1, 2] = -0.75, 0.75
    rows[count - 2, count - 3], rows[count - 2, count - 1] = -0.75, 0.75
    rows[count - 1, count - 3:] = (-0.5, -2.0, 2.5)
    return rows


def dense_derivative(count):
    lower, upper = diagonals(count)
    matrix = np.eye(count) + np.diag(lower[1:], -1) + np.diag(upper[:-1], 1)
    return np.linalg.solve(matrix, stencil(count))


class Table:
    def __init__(self, blocks, cells):
        count = blocks * cells
        lower, upper = diagonals(count)
        rows = stencil(count)
        down, pivot = np.zeros(count), np.ones(count)
        for i in range(1, count):
            down[i] = lower[i] / pivot[i - 1]
            pivot[i] = 1.0 - down[i] * upper[i - 1]
        up, pivot_up = np.zeros(count), np.ones(count)
        for i in range(count - 2, -1, -1):
            up[i] = upper[i] / pivot_up[i + 1]
            pivot_up[i] = 1.0 - up[i] * lower[i + 1]
        from_left = rows.copy()
        for i in range(1, count):
            from_left[i] -= down[i] * from_left[i - 1]
        from_right = rows.copy()
        for i in range(count - 2, -1, -1):
            from_right[i] -= up[i] * from_right[i + 1]
        part = {
            "right": np.zeros((blocks, cells)), "left": np.zeros((blocks, cells)),
            "near": np.zeros((blocks, cells)), "wide": np.zeros((blocks, cells)),
            "back": np.zeros((blocks, cells)), "ahead": np.zeros((blocks, cells)),
            "edge": np.zeros((blocks, 4, 4)), "link": np.zeros((blocks, 4)),
            "ends": np.zeros((blocks, 4)),
        }
        chain = np.zeros((blocks, 2))
        for d in range(blocks):
            s, e = d * cells, (d + 1) * cells
            if d < blocks - 1:
                part["right"][d] = from_left[e + 1, s:e]
                chain[d, 0] = np.prod(-down[s + 2:e + 2])
            if d > 0:
                part["left"][d] = from_right[s - 2, s:e]
                chain[d, 1] = np.prod(-up[s - 2:e - 2])
            inverse = 1.0 / pivot[s:e]
            inverse[-1] = 1.0 / (pivot[e - 1] + pivot_up[e - 1] - 1.0)
            part["near"][d] = 7.0 / 9.0 * inverse
            part["wide"][d] = 1.0 / 36.0 * inverse
            part["back"][d] = lower[s:e] * inverse
            part["ahead"][d] = upper[s:e] / pivot[s:e]
            part["edge"][d, 0, :3] = from_left[s, s:s + 3] * inverse[0]
            part["edge"][d, 1] = rows[s + 1, s:s + 4] * inverse[1]
            part["edge"][d, 2] = rows[e - 2, e - 4:e] * inverse[-2]
            part["edge"][d, 3, 1:] = from_right[e - 1, e - 3:e] * inverse[-1]
            part["ends"][d, 0] = -inverse[0] / down[s + 1]
            part["ends"][d, 1] = -inverse[-1] / up[e - 2]
            if d > 0:
                part["ends"][d, 2] = rows[s + 1, s - 1] / lower[s + 1]
            if d < blocks - 1:
                part["ends"][d, 3] = rows[e - 2, e] / upper[e - 2]
        part["link"][1:, 0] = chain[1:, 0] * chain[:-1, 0]
        part["link"][:-1, 1] = chain[:-1, 1] * chain[1:, 1]
        part["link"][1:, 2] = chain[:-1, 0]
        part["link"][:-1, 3] = chain[1:, 1]
        largest, hops, reach = np.abs(chain).max(), 1, np.abs(chain).max()
        while hops < blocks - 1 and reach >= np.finfo(np.float32).tiny:
            hops, reach = hops + 1, reach * largest
        assert hops <= 3
        self.at, column = {}, 0
        for name, values in part.items():
            self.at[name] = column
            column += values[0].size
        self.stride = column
        self.values = np.concatenate(
            [values.reshape(blocks, -1) for values in part.values()], axis=1
        ).astype(np.float32).reshape(-1)


def quotient(largest, divisor):
    for shift in range(31):
        factor = -(-(1 << shift) // divisor)
        excess = factor * divisor - (1 << shift)
        if excess * (largest - 1) < (1 << shift) and factor * (largest - 1) < 2**31:
            return factor, shift
    raise AssertionError("no factor")


def fused_kernel(
    sizes, where, stride,
    table_ref, cell_ref, state_ref, flow_ref, zhi_in, zlo_in,
    cells_ref, normal_ref, pos_ref, observer_ref, bin_in,
    next_ref, signal_ref,
    zhi_ref, zlo_ref, bin_ref, pad, plain, base, swept, rate,
    to_right, to_left, left_sum, right_sum, on_right, on_left, far_left, far_right,
    left_plane, right_plane,
    geometry, kernels, picked, contribution, binned, pieces, landing,
    lines, chosen, ask, asked, reply, got, mends, columns_ref, own_ref,
    load_sem, halo_send, halo_recv, plane_send, plane_recv, sum_send, sum_recv,
    piece_send, piece_recv, ask_send, ask_recv, reply_send, reply_recv,
):
    blocks, groups = sizes
    _, cells, width, depth = next_ref.shape
    faces, observers = bin_ref.shape
    tiles, halves, count = width // TILE, depth // LANES, blocks * groups
    block, group = lax.axis_index("gx"), lax.axis_index("yz")
    me = block * groups + group
    row0 = block * stride

    def scalar(name, i=0):
        return table_ref[row0 + (where[name] + i)]

    place = {"gx": (block, blocks), "yz": (group, groups)}

    def there(axis, shift):
        index, number = place[axis]
        return index + shift < number if shift > 0 else index + shift >= 0

    def other(axis, shift):
        index, number = place[axis]
        return {axis: jnp.clip(index + shift, 0, number - 1)}

    def partner(k):
        index = lax.rem(me + k, count)
        return {"gx": lax.div(index, groups), "yz": lax.rem(index, groups)}, index

    loads = []
    for slot, f in enumerate(PADDED):
        source = flow_ref if f == 4 else state_ref.at[f]
        for h in range(halves):
            loads.append(pltpu.make_async_copy(
                source.at[:, :, h * LANES:(h + 1) * LANES],
                pad.at[slot, h, :, TILE:TILE + width, :], load_sem.at[len(loads)],
            ))
    for slot, f in enumerate(PLAIN):
        loads.append(pltpu.make_async_copy(state_ref.at[f], plain.at[slot], load_sem.at[len(loads)]))
    spare = [
        pltpu.make_async_copy(source, target, load_sem.at[len(loads) + k])
        for k, (source, target) in enumerate(((zhi_in, zhi_ref), (zlo_in, zlo_ref), (bin_in, bin_ref)))
    ]
    for load in loads + spare:
        load.start()

    barrier = pltpu.get_barrier_semaphore()
    for k in range(1, count):
        pl.semaphore_signal(barrier, inc=1, device_id=partner(k)[0], device_id_type=MESH)

    for axis, shift, targets in (
        ("gx", -1, (left_sum, left_plane, asked.at[0], got.at[0])),
        ("gx", 1, (right_sum, right_plane, asked.at[1], got.at[1])),
        ("gx", -2, (far_left,)), ("gx", 2, (far_right,)),
    ):
        @pl.when(jnp.logical_not(there(axis, shift)))
        def _():
            for target in targets:
                target[...] = jnp.zeros_like(target)
    for shift, at in ((-1, TILE - REACH), (1, TILE + width)):
        @pl.when(jnp.logical_not(there("yz", shift)))
        def _():
            pad[:, :, :, at:at + REACH, :] = jnp.zeros((len(PADDED), halves, cells, REACH, LANES), jnp.float32)

    def remote(source, target, send, recv, axis, shift):
        return pltpu.make_async_remote_copy(
            src_ref=source, dst_ref=target, send_sem=send, recv_sem=recv,
            device_id=other(axis, shift), device_id_type=MESH,
        )

    def start(copy, axis, shift):
        @pl.when(there(axis, shift))
        def _():
            copy.start()

    def arrive(copy, axis, shift):
        @pl.when(there(axis, -shift))
        def _():
            copy.wait_recv()

    def sent(copy, axis, shift):
        @pl.when(there(axis, shift))
        def _():
            copy.wait_send()

    def near(side, t):
        if side == 0:
            return remote(on_right.at[t], left_sum.at[t], sum_send.at[0, t], sum_recv.at[0, t], "gx", 1), "gx", 1
        return remote(on_left.at[t], right_sum.at[t], sum_send.at[1, t], sum_recv.at[1, t], "gx", -1), "gx", -1

    def far(side, t):
        if side == 0:
            return remote(to_right.at[t], far_left.at[t], sum_send.at[2, t], sum_recv.at[2, t], "gx", 2), "gx", 2
        return remote(to_left.at[t], far_right.at[t], sum_send.at[3, t], sum_recv.at[3, t], "gx", -2), "gx", -2

    halos = [
        (remote(pad.at[:, :, :, TILE + width - REACH:TILE + width, :], pad.at[:, :, :, TILE - REACH:TILE, :],
                halo_send.at[0], halo_recv.at[0], "yz", 1), "yz", 1),
        (remote(pad.at[:, :, :, TILE:TILE + REACH, :], pad.at[:, :, :, TILE + width:TILE + width + REACH, :],
                halo_send.at[1], halo_recv.at[1], "yz", -1), "yz", -1),
    ]
    planes = [[], []]
    for side, (at, target, shift) in enumerate(((cells - 1, left_plane, 1), (0, right_plane, -1))):
        for piece, (source, into) in enumerate((
            (state_ref.at[0:2, at], target.at[0:2]), (state_ref.at[2:4, at], target.at[2:4]),
            (flow_ref.at[at], target.at[4]),
        )):
            planes[0 if piece in EARLY else 1].append((remote(
                source, into, plane_send.at[side, piece], plane_recv.at[side, piece], "gx", shift
            ), "gx", shift))

    def value(f, i, rows, h):
        if f in PADDED:
            return pad[PADDED.index(f), h, i, pl.ds(rows + TILE, TILE), :]
        return plain[PLAIN.index(f), i, pl.ds(rows, TILE), h * LANES:(h + 1) * LANES]

    def first_row(t):
        return pl.multiple_of(t * TILE, TILE)

    factor, shift = quotient(cells * width * groups, width * groups)
    power = depth.bit_length() - 1
    origin = block * (cells * width * groups)

    def locate(cell):
        line = (cell >> power if depth & (depth - 1) == 0 else lax.div(cell, depth)) - origin
        along_x = (line * factor) >> shift
        return along_x, line - along_x * (width * groups) - group * width

    ask[...] = jnp.full_like(ask, -1.0)
    along_x, along_y = locate(cells_ref[...])
    along_z = cells_ref[...] & (depth - 1) if depth & (depth - 1) == 0 else lax.rem(cells_ref[...], depth)
    for k, along in enumerate((along_y, along_z, along_x)):
        ask[k:k + 1, 0:faces] = along.astype(jnp.float32)
    asks = [
        (remote(ask, asked.at[0], ask_send.at[0], ask_recv.at[0], "gx", 1), "gx", 1),
        (remote(ask, asked.at[1], ask_send.at[1], ask_recv.at[1], "gx", -1), "gx", -1),
    ]
    replies = [
        (remote(reply.at[0], got.at[1], reply_send.at[0], reply_recv.at[0], "gx", -1), "gx", -1),
        (remote(reply.at[1], got.at[0], reply_send.at[1], reply_recv.at[1], "gx", 1), "gx", 1),
    ]

    pl.semaphore_wait(barrier, count - 1)
    for entry in asks:
        start(*entry)
    for entry in planes[0]:
        start(*entry)
    for load in loads[:len(PADDED) * halves]:
        load.wait()
    for entry in halos:
        start(*entry)
    for load in loads[len(PADDED) * halves:] + spare:
        load.wait()

    fields = range(5)
    pairs = [(f, h) for f in fields for h in range(halves)]

    def sums(t, carry):
        rows = first_row(t)
        totals = None
        for i in range(cells):
            weights = scalar("right", i), scalar("left", i)
            now = [value(f, i, rows, h) for f, h in pairs]
            terms = [[weight * one for weight in weights] for one in now]
            totals = terms if totals is None else [
                [old + new for old, new in zip(*both)] for both in zip(totals, terms)
            ]
        for (f, h), (total_right, total_left) in zip(pairs, totals):
            lanes = slice(h * LANES, (h + 1) * LANES)
            to_right[t, f, :, lanes] = total_right
            to_left[t, f, :, lanes] = total_left
        start(*far(0, t))
        start(*far(1, t))
        return carry

    lax.fori_loop(0, tiles, sums, 0)

    def relay(t):
        arrive(*far(0, t))
        arrive(*far(1, t))
        on_right[t] = to_right[t] + scalar("link", 0) * far_left[t]
        on_left[t] = to_left[t] + scalar("link", 1) * far_right[t]
        start(*near(0, t))
        start(*near(1, t))


    together = 4 if cells % 4 == 0 else 1

    def multiply(k, carry):
        span = pl.ds(k * together, together)
        for f, target in ((0, 3), (3, 0), (4, 1)):
            if f in PADDED:
                lines = jnp.concatenate([
                    pad[PADDED.index(f), h, span, TILE:TILE + width, :].reshape(together * width, LANES)
                    for h in range(halves)
                ], axis=1)
            else:
                lines = plain[PLAIN.index(f), span].reshape(together * width, depth)
            high = lines.astype(jnp.bfloat16)
            rest = (lines - high.astype(jnp.float32)).astype(jnp.bfloat16)
            out = jnp.dot(rest, zhi_ref[...], preferred_element_type=jnp.float32)
            out += jnp.dot(high, zlo_ref[...], preferred_element_type=jnp.float32)
            out += jnp.dot(high, zhi_ref[...], preferred_element_type=jnp.float32)
            base[target, span] = out.reshape(together, width, depth)
        return carry

    steps = cells // together
    lax.fori_loop(0, steps // 2, multiply, 0)
    relay(0)
    lax.fori_loop(steps // 2, steps, multiply, 0)

    for entry in halos:
        arrive(*entry)

    def lateral(i, carry):
        for t in range(tiles):
            rows = t * TILE
            for h in range(halves):
                lanes = slice(h * LANES, (h + 1) * LANES)

                def y_rate(slot):
                    def take(shift):
                        return pad[slot, h, i, TILE + rows + shift:2 * TILE + rows + shift, :]
                    return (
                        0.75 * (take(1) - take(-1)) - 0.15 * (take(2) - take(-2))
                        + 1.0 / 60.0 * (take(3) - take(-3))
                    )

                spot = (i, slice(rows, rows + TILE), lanes)
                base[(0,) + spot] = base[(0,) + spot] + y_rate(1)
                base[(1,) + spot] = value(2, i, rows, h) * y_rate(2) + value(3, i, rows, h) * base[(1,) + spot]
                base[(2,) + spot] = y_rate(0)
        return carry

    pumps = max(tiles - 1, 1)
    for t in range(pumps):
        if t + 1 < tiles:
            relay(t + 1)
        lax.fori_loop(cells * t // pumps, cells * (t + 1) // pumps, lateral, 0)

    def plane_of(f, i):
        if f in PADDED:
            return jnp.concatenate(
                [pad[PADDED.index(f), h, i, TILE:TILE + width, :] for h in range(halves)], axis=1
            )
        return plain[PLAIN.index(f), i]

    def gather_columns(values, places):
        ahead = lax.broadcasted_iota(jnp.int32, (depth, places.shape[1]), 0).astype(jnp.float32)
        hot = jnp.where(ahead == places[1:2, :], 1.0, 0.0).astype(jnp.bfloat16)
        rest, total = jnp.concatenate(values, axis=0), None
        for _ in range(3):
            part = rest.astype(jnp.bfloat16)
            rest = rest - part.astype(jnp.float32)
            product = jnp.dot(part, hot, preferred_element_type=jnp.float32)
            total = product if total is None else total + product
        here = lax.broadcasted_iota(jnp.int32, (width, places.shape[1]), 0).astype(jnp.float32) == places[0:1, :]
        return [
            jnp.sum(jnp.where(here, total[k * width:(k + 1) * width], 0.0), axis=0, keepdims=True)
            for k in range(len(values))
        ]

    reply[...] = jnp.zeros_like(reply)
    for side, at in ((0, 0), (1, cells - 1)):
        arrive(*asks[side])
        for k, row in enumerate(gather_columns([plane_of(f, at) for f in fields], asked[side])):
            reply[side, k:k + 1, :] = row
        start(*replies[side])
    own = gather_columns([plane_of(f, at) for at in (0, cells - 1) for f in (1, 4)], ask[...])

    def find(k, carry):
        along_x, along_y = locate(cell_ref[k])
        along_x, along_y = jnp.clip(along_x, 0, cells - 1), jnp.clip(along_y, 0, width - 1)
        lines[k] = along_x * width + along_y
        for h in range(halves):
            chosen[h, pl.ds(k, 1), :] = pad[0, h, along_x, pl.ds(TILE + along_y, 1), :]
        return carry

    lax.fori_loop(0, faces, find, 0, unroll=4)

    geometry[...] = jnp.zeros_like(geometry)
    geometry[0:3, 0:faces] = normal_ref[...]
    geometry[3:6, 0:faces] = pos_ref[...]
    geometry[6:7, 0:faces] = along_z.astype(jnp.float32)
    columns_ref[...] = geometry[...].T

    def column(c):
        return columns_ref[0:faces, c:c + 1]

    normal = [column(c) for c in range(3)]
    offset = [observer_ref[c:c + 1, :] - column(3 + c) for c in range(3)]
    distance = jnp.sqrt(offset[0] * offset[0] + offset[1] * offset[1] + offset[2] * offset[2])
    normal_r = (normal[0] * offset[0] + normal[1] * offset[1] + normal[2] * offset[2]) / distance
    scale = 1.0 / (four_pi * distance)
    kernels[0] = scale
    kernels[1] = normal_r * scale
    kernels[2] = normal_r * scale / distance
    mask = lax.broadcasted_iota(jnp.int32, (faces, depth), 1) == column(6).astype(jnp.int32)
    nearby = jnp.concatenate([chosen[h] for h in range(halves)], axis=1)
    columns_ref[0:faces, 7:8] = jnp.sum(jnp.where(mask, nearby, 0.0), axis=1, keepdims=True)
    own_ref[...] = jnp.zeros_like(own_ref)
    for k, row in enumerate(own):
        own_ref[k:k + 1, :] = row

    chunk = 4
    assert cells % chunk == 0 and cells >= 3 * chunk

    def finish(t):
        rows = first_row(t)
        n = cells
        carry = []
        edge = [scalar("edge", j) for j in range(8)]
        link, end, back = scalar("link", 2), scalar("ends", 0), scalar("back", 1)
        for f, h in pairs:
            lanes = slice(h * LANES, (h + 1) * LANES)
            own = [value(f, i, rows, h) for i in range(4)]
            incoming = left_sum[t, f, :, lanes] + link * far_left[t, f, :, lanes]
            first = edge[0] * own[0] + edge[1] * own[1] + edge[2] * own[2] + end * incoming
            second = edge[4] * own[0] + edge[5] * own[1] + edge[6] * own[2] + edge[7] * own[3] - back * first
            swept[f, 0, :, lanes] = first
            swept[f, 1, :, lanes] = second
            carry.append(second)

        def forward(k, carry):
            i0 = 2 + k * chunk
            new = list(carry)
            factors = [[scalar(name, i0 + j) for name in ("near", "wide", "back")] for j in range(chunk)]
            for p, (f, h) in enumerate(pairs):
                lanes = slice(h * LANES, (h + 1) * LANES)
                own = [value(f, i0 + j, rows, h) for j in range(-2, chunk + 2)]
                for j in range(chunk):
                    close, wide, back = factors[j]
                    new[p] = close * (own[j + 3] - own[j + 1]) + wide * (own[j + 4] - own[j]) - back * new[p]
                    swept[f, i0 + j, :, lanes] = new[p]
            return tuple(new)

        carry = lax.fori_loop(0, (n - 4) // chunk, forward, tuple(carry))
        solved = []
        edge = [scalar("edge", 8 + j) for j in range(8)]
        link, end, back, last = scalar("link", 3), scalar("ends", 1), scalar("back", n - 2), scalar("back", n - 1)
        for p, (f, h) in enumerate(pairs):
            lanes = slice(h * LANES, (h + 1) * LANES)
            own = [value(f, i, rows, h) for i in range(n - 4, n)]
            incoming = right_sum[t, f, :, lanes] + link * far_right[t, f, :, lanes]
            before = (
                edge[0] * own[0] + edge[1] * own[1] + edge[2] * own[2] + edge[3] * own[3] - back * carry[p]
            )
            swept[f, n - 2, :, lanes] = before
            solved.append(
                edge[5] * own[1] + edge[6] * own[2] + edge[7] * own[3] + end * incoming - last * before
            )

        def store(i, x):
            spot = pl.ds(pl.multiple_of(i * width + rows, TILE), TILE)
            for h in range(halves):
                lanes = slice(h * LANES, (h + 1) * LANES)
                old = [value(f, i, rows, h) for f in fields]
                flow = old[4]
                px, ux, vx, wx, fx = (x[f * halves + h] for f in fields)
                terms = [base[c, i, pl.ds(rows, TILE), lanes] for c in range(4)]
                losses = (
                    flow * px + ux + terms[0],
                    flow * ux + old[1] * fx + px + terms[1],
                    flow * vx + terms[2],
                    flow * wx + terms[3],
                )
                for c in range(4):
                    rate[c, spot, lanes] = losses[c]
                    next_ref[c, i, pl.ds(rows, TILE), lanes] = old[c] - time_step * losses[c]

        def step_back(i, x):
            ahead = scalar("ahead", i)
            x = [
                swept[f, i, :, h * LANES:(h + 1) * LANES] - ahead * x[p]
                for p, (f, h) in enumerate(pairs)
            ]
            store(i, x)
            return x

        store(n - 1, solved)
        for j in range(2, chunk + 1):
            solved = step_back(n - j, solved)

        def backward(k, x):
            for j in range(chunk):
                x = step_back(n - chunk - 1 - k * chunk - j, x)
            return tuple(x)

        lax.fori_loop(0, n // chunk - 1, backward, tuple(solved))

    def main(t, carry):
        arrive(*near(0, t))
        arrive(*near(1, t))

        @pl.when(t == max(tiles - 2, 0))
        def _():
            for entry in planes[1]:
                start(*entry)

        finish(t)
        return carry

    lax.fori_loop(0, tiles, main, 0)

    for entry in replies:
        arrive(*entry)
    along = ask[2:3, :]
    first, last = along == 0.0, along == float(cells - 1)
    more = [
        jnp.where(first, scalar("ends", 2) * got[0, f:f + 1, :], 0.0)
        + jnp.where(last, scalar("ends", 3) * got[1, f:f + 1, :], 0.0) for f in fields
    ]
    stream, flow = (jnp.where(first, own_ref[k:k + 1, :], own_ref[2 + k:3 + k, :]) for k in range(2))
    mends[...] = jnp.zeros_like(mends)
    for c, row in enumerate((
        flow * more[0] + more[1], flow * more[1] + stream * more[4] + more[0], flow * more[2], flow * more[3],
    )):
        mends[c:c + 1, :] = row
    mended = mends[...].T

    def pick(k, carry):
        row = lines[k]
        for c in range(4):
            picked[c, pl.ds(k, 1), :] = rate[c, pl.ds(row, 1), :]
        return carry

    lax.fori_loop(0, faces, pick, 0, unroll=4)
    mask = lax.broadcasted_iota(jnp.int32, (faces, depth), 1) == column(6).astype(jnp.int32)
    at = [
        jnp.sum(jnp.where(mask, picked[c], 0.0), axis=1, keepdims=True) + mended[0:faces, c:c + 1] for c in range(4)
    ]
    pressure = column(7) - time_step * at[0]
    normal_rate = column(0) * at[1] + column(1) * at[2] + column(2) * at[3]
    contribution[...] = pressure * kernels[2] - at[0] * kernels[1] - normal_rate * kernels[0]

    def gather(k, carry):
        b0 = pl.multiple_of(k * TILE, TILE)
        for o in range(observers // LANES):
            lanes = slice(o * LANES, (o + 1) * LANES)
            totals = [jnp.zeros((TILE, LANES), jnp.float32)] * TILE
            for r in range(0, faces, TILE):
                bins, parts = bin_ref[r:r + TILE, lanes], contribution[r:r + TILE, lanes]
                totals = [
                    total + jnp.where(bins == b0 + j, parts, 0.0) for j, total in enumerate(totals)
                ]
            binned[pl.ds(b0, TILE), lanes] = jnp.concatenate(
                [jnp.sum(total, axis=0, keepdims=True) for total in totals], axis=0
            )
        return carry

    lax.fori_loop(0, BINS // TILE, gather, 0)
    share, beside = observers // count, LANES // BINS
    dense = share % (TILE * beside) == 0
    if not dense:
        pieces[...] = jnp.zeros_like(pieces)
    turned = jnp.concatenate([binned[...], jnp.zeros((LANES - BINS, observers), jnp.float32)], axis=0).T
    if dense:
        turned = turned.reshape(count, share // TILE, TILE, LANES)
        lane = lax.broadcasted_iota(jnp.int32, (count * TILE, LANES), 1)
        for q in range(share // TILE // beside):
            row = turned[:, q * beside].reshape(count * TILE, LANES)
            for j in range(1, beside):
                moved = pltpu.roll(turned[:, q * beside + j].reshape(count * TILE, LANES), j * BINS, 1)
                row = jnp.where(lane >= j * BINS, moved, row)
            pieces[:, q] = row.reshape(count, TILE, LANES)
    else:
        for d in range(count):
            pieces[d, 0, 0:share, :] = turned[d * share:(d + 1) * share]
    copies = []
    for k in range(1, count):
        target, index = partner(k)
        copies.append(pltpu.make_async_remote_copy(
            src_ref=pieces.at[index], dst_ref=landing.at[k - 1],
            send_sem=piece_send.at[k - 1], recv_sem=piece_recv.at[k - 1],
            device_id=target, device_id_type=MESH,
        ))
        copies[-1].start()
    for entry in planes[0] + planes[1]:
        arrive(*entry)

    def mend(t, carry):
        rows = first_row(t)
        for at, plane, end in ((0, left_plane, 2), (cells - 1, right_plane, 3)):
            spot = pl.ds(pl.multiple_of(at * width + rows, TILE), TILE)
            for h in range(halves):
                lanes = slice(h * LANES, (h + 1) * LANES)
                px, ux, vx, wx, fx = (scalar("ends", end) * plane[f, pl.ds(rows, TILE), lanes] for f in fields)
                stream, flow = value(1, at, rows, h), value(4, at, rows, h)
                more = (flow * px + ux, flow * ux + stream * fx + px, flow * vx, flow * wx)
                for c in range(4):
                    rate[c, spot, lanes] = rate[c, spot, lanes] + more[c]
                    next_ref[c, at, pl.ds(rows, TILE), lanes] = (
                        next_ref[c, at, pl.ds(rows, TILE), lanes] - time_step * more[c]
                    )
        return carry

    lax.fori_loop(0, tiles, mend, 0)

    total = pieces[me]
    for k in range(count - 1):
        copies[k].wait_recv()
        total += landing[k]
    if dense:
        for q in range(share // TILE // beside):
            for j in range(beside):
                moved = total[q] if j == 0 else pltpu.roll(total[q], LANES - j * BINS, 1)
                top = (q * beside + j) * TILE
                signal_ref[top:top + TILE, :] = moved[:, 0:BINS]
    else:
        signal_ref[...] = total[0, 0:share, 0:BINS]

    for k in range(count - 1):
        copies[k].wait_send()
    for entry in halos + planes[0] + planes[1] + asks + replies:
        sent(*entry)

    def drain(t, carry):
        for side in (0, 1):
            sent(*near(side, t))
            sent(*far(side, t))
        return carry

    lax.fori_loop(0, tiles, drain, 0)


def copy_kernel(next_ref, signal_ref, next_out, signal_out, sems):
    copies = [
        pltpu.make_async_copy(next_ref, next_out, sems.at[0]),
        pltpu.make_async_copy(signal_ref, signal_out, sems.at[1]),
    ]
    for copy in copies:
        copy.start()
    for copy in copies:
        copy.wait()


def per_device(sizes, state, mean_flow, face_cell, face_normal, face_pos, observer_pos, time_bin):
    blocks, groups = sizes
    _, cells, width, depth = state.shape
    faces, observers = time_bin.shape
    tiles, halves, devices = width // TILE, depth // LANES, blocks * groups
    share = observers // devices
    dense = share % (TILE * (LANES // BINS)) == 0
    packed = (share * BINS // (TILE * LANES), TILE, LANES) if dense else (1, -(-share // TILE) * TILE, LANES)
    table = Table(blocks, cells)
    operator = dense_derivative(depth).T.astype(np.float32)
    z_high = jnp.asarray(operator).astype(jnp.bfloat16)
    z_low = (jnp.asarray(operator) - z_high.astype(jnp.float32)).astype(jnp.bfloat16)
    f32 = jnp.float32
    padded_faces = -(-faces // LANES) * LANES
    smem, vmem, hbm = (pl.BlockSpec(memory_space=space) for space in (SMEM, VMEM, HBM))
    dma = pltpu.SemaphoreType.DMA
    sums = VMEM((tiles, 5, TILE, depth), f32)
    state_next, signal = pl.pallas_call(
        functools.partial(fused_kernel, sizes, table.at, table.stride),
        out_shape=(VMEM(state.shape, f32), VMEM((share, BINS), f32)),
        in_specs=[smem, smem, hbm, hbm, hbm, hbm, vmem, vmem, vmem, vmem, hbm],
        out_specs=(vmem, vmem),
        scratch_shapes=[
            VMEM((depth, depth), jnp.bfloat16), VMEM((depth, depth), jnp.bfloat16),
            VMEM((faces, observers), jnp.int32),
            VMEM((len(PADDED), halves, cells, width + 2 * TILE, LANES), f32),
            VMEM((len(PLAIN), cells, width, depth), f32),
            VMEM((4, cells, width, depth), f32),
            VMEM((5, cells, TILE, depth), f32),
            VMEM((4, cells * width, depth), f32),
        ] + [sums] * 8 + [
            VMEM((5, width, depth), f32), VMEM((5, width, depth), f32),
            VMEM((TILE, padded_faces), f32), VMEM((3, faces, observers), f32),
            VMEM((4, faces, depth), f32), VMEM((faces, observers), f32),
            VMEM((BINS, observers), f32), VMEM((devices,) + packed, f32),
            VMEM((devices - 1,) + packed, f32),
            SMEM((faces,), jnp.int32), VMEM((halves, faces, LANES), f32), VMEM((TILE, padded_faces), f32), VMEM((2, TILE, padded_faces), f32),
            VMEM((2, TILE, padded_faces), f32), VMEM((2, TILE, padded_faces), f32),
            VMEM((TILE, padded_faces), f32), VMEM((padded_faces, TILE), f32), VMEM((TILE, padded_faces), f32),
            dma((len(PADDED) * halves + len(PLAIN) + 3,)), dma((2,)), dma((2,)), dma((2, 3)), dma((2, 3)),
            dma((4, tiles)), dma((4, tiles)), dma((devices - 1,)), dma((devices - 1,)),
            dma((2,)), dma((2,)), dma((2,)), dma((2,)),
        ],
        compiler_params=pltpu.CompilerParams(
            collective_id=0, has_side_effects=True, vmem_limit_bytes=VMEM_MIB * 1024 * 1024
        ),
    )(
        jnp.asarray(table.values), face_cell, state, mean_flow, z_high, z_low,
        face_cell.reshape(1, faces), face_normal, face_pos, observer_pos, time_bin,
    )
    return pl.pallas_call(
        copy_kernel,
        out_shape=(
            jax.ShapeDtypeStruct(state.shape, f32),
            jax.ShapeDtypeStruct((share, BINS), f32),
        ),
        in_specs=[vmem, vmem],
        out_specs=(hbm, hbm),
        scratch_shapes=[dma((2,))],
        compiler_params=pltpu.CompilerParams(vmem_limit_bytes=8 * 1024 * 1024),
    )(state_next, signal)


def solution(mesh):
    in_specs = (
        P(None, "gx", "yz", None),
        P("gx", "yz", None),
        P(("gx", "yz")),
        P(None, ("gx", "yz")),
        P(None, ("gx", "yz")),
        P(),
        P(("gx", "yz"), None),
    )
    out_specs = (P(None, "gx", "yz", None), P(("gx", "yz"), None))
    sizes = (mesh.shape["gx"], mesh.shape["yz"])
    return jax.shard_map(
        functools.partial(per_device, sizes),
        mesh=mesh, in_specs=in_specs, out_specs=out_specs, check_vma=False,
    )
```

```python
import functools

import numpy as np
import jax
import jax.numpy as jnp
from jax import lax
from jax.experimental import pallas as pl
from jax.experimental.pallas import tpu as pltpu
from jax.sharding import PartitionSpec as P

BINS = 64
TILE = 8
LANES = 128
REACH = 3
VMEM_MIB = 54
EARLY = (0, 2)

time_step = 0.25
four_pi = 4.0 * 3.141592653589793
VMEM = pltpu.VMEM
SMEM = pltpu.SMEM
HBM = pltpu.HBM
MESH = pl.DeviceIdType.MESH

PADDED = (0, 2, 4)
PLAIN = (1, 3)


def diagonals(count):
    lower = np.full(count, 1.0 / 3.0)
    upper = np.full(count, 1.0 / 3.0)
    lower[1] = lower[count - 2] = upper[1] = upper[count - 2] = 0.25
    lower[0] = upper[count - 1] = 0.0
    lower[count - 1] = upper[0] = 2.0
    return lower, upper


def stencil(count):
    rows = np.zeros((count, count))
    for i in range(2, count - 2):
        rows[i, i + 1], rows[i, i - 1] = 7.0 / 9.0, -7.0 / 9.0
        rows[i, i + 2], rows[i, i - 2] = 1.0 / 36.0, -1.0 / 36.0
    rows[0, :3] = (-2.5, 2.0, 0.5)
    rows[1, 0], rows[1, 2] = -0.75, 0.75
    rows[count - 2, count - 3], rows[count - 2, count - 1] = -0.75, 0.75
    rows[count - 1, count - 3:] = (-0.5, -2.0, 2.5)
    return rows


def dense_derivative(count):
    lower, upper = diagonals(count)
    matrix = np.eye(count) + np.diag(lower[1:], -1) + np.diag(upper[:-1], 1)
    return np.linalg.solve(matrix, stencil(count))


class Table:
    def __init__(self, blocks, cells):
        count = blocks * cells
        lower, upper = diagonals(count)
        rows = stencil(count)
        down, pivot = np.zeros(count), np.ones(count)
        for i in range(1, count):
            down[i] = lower[i] / pivot[i - 1]
            pivot[i] = 1.0 - down[i] * upper[i - 1]
        up, pivot_up = np.zeros(count), np.ones(count)
        for i in range(count - 2, -1, -1):
            up[i] = upper[i] / pivot_up[i + 1]
            pivot_up[i] = 1.0 - up[i] * lower[i + 1]
        from_left = rows.copy()
        for i in range(1, count):
            from_left[i] -= down[i] * from_left[i - 1]
        from_right = rows.copy()
        for i in range(count - 2, -1, -1):
            from_right[i] -= up[i] * from_right[i + 1]
        part = {
            "right": np.zeros((blocks, cells)), "left": np.zeros((blocks, cells)),
            "near": np.zeros((blocks, cells)), "wide": np.zeros((blocks, cells)),
            "back": np.zeros((blocks, cells)), "ahead": np.zeros((blocks, cells)),
            "edge": np.zeros((blocks, 4, 4)), "link": np.zeros((blocks, 4)),
            "ends": np.zeros((blocks, 4)),
        }
        chain = np.zeros((blocks, 2))
        for d in range(blocks):
            s, e = d * cells, (d + 1) * cells
            if d < blocks - 1:
                part["right"][d] = from_left[e + 1, s:e]
                chain[d, 0] = np.prod(-down[s + 2:e + 2])
            if d > 0:
                part["left"][d] = from_right[s - 2, s:e]
                chain[d, 1] = np.prod(-up[s - 2:e - 2])
            inverse = 1.0 / pivot[s:e]
            inverse[-1] = 1.0 / (pivot[e - 1] + pivot_up[e - 1] - 1.0)
            part["near"][d] = 7.0 / 9.0 * inverse
            part["wide"][d] = 1.0 / 36.0 * inverse
            part["back"][d] = lower[s:e] * inverse
            part["ahead"][d] = upper[s:e] / pivot[s:e]
            part["edge"][d, 0, :3] = from_left[s, s:s + 3] * inverse[0]
            part["edge"][d, 1] = rows[s + 1, s:s + 4] * inverse[1]
            part["edge"][d, 2] = rows[e - 2, e - 4:e] * inverse[-2]
            part["edge"][d, 3, 1:] = from_right[e - 1, e - 3:e] * inverse[-1]
            part["ends"][d, 0] = -inverse[0] / down[s + 1]
            part["ends"][d, 1] = -inverse[-1] / up[e - 2]
            if d > 0:
                part["ends"][d, 2] = rows[s + 1, s - 1] / lower[s + 1]
            if d < blocks - 1:
                part["ends"][d, 3] = rows[e - 2, e] / upper[e - 2]
        part["link"][1:, 0] = chain[1:, 0] * chain[:-1, 0]
        part["link"][:-1, 1] = chain[:-1, 1] * chain[1:, 1]
        part["link"][1:, 2] = chain[:-1, 0]
        part["link"][:-1, 3] = chain[1:, 1]
        largest, hops, reach = np.abs(chain).max(), 1, np.abs(chain).max()
        while hops < blocks - 1 and reach >= np.finfo(np.float32).tiny:
            hops, reach = hops + 1, reach * largest
        assert hops <= 3
        self.at, column = {}, 0
        for name, values in part.items():
            self.at[name] = column
            column += values[0].size
        self.stride = column
        self.values = np.concatenate(
            [values.reshape(blocks, -1) for values in part.values()], axis=1
        ).astype(np.float32).reshape(-1)


def quotient(largest, divisor):
    for shift in range(31):
        factor = -(-(1 << shift) // divisor)
        excess = factor * divisor - (1 << shift)
        if excess * (largest - 1) < (1 << shift) and factor * (largest - 1) < 2**31:
            return factor, shift
    raise AssertionError("no factor")


def fused_kernel(
    sizes, where, stride,
    table_in, cell_in, state_ref, flow_ref, zhi_in, zlo_in,
    cells_in, normal_in, pos_in, observer_in, bin_in,
    next_ref, signal_ref,
    table_ref, cell_ref, cells_ref, normal_ref, pos_ref, observer_ref, zhi_ref, zlo_ref, bin_ref, pad, plain, base, swept, rate,
    to_right, to_left, left_sum, right_sum, on_right, on_left, far_left, far_right,
    left_plane, right_plane,
    geometry, kernels, picked, contribution, binned, pieces, landing,
    lines, chosen, ask, asked, reply, got, mends, columns_ref, own_ref,
    load_sem, halo_send, halo_recv, plane_send, plane_recv, sum_send, sum_recv,
    piece_send, piece_recv, ask_send, ask_recv, reply_send, reply_recv,
):
    blocks, groups = sizes
    _, cells, width, depth = next_ref.shape
    faces, observers = bin_ref.shape
    tiles, halves, count = width // TILE, depth // LANES, blocks * groups
    block, group = lax.axis_index("gx"), lax.axis_index("yz")
    me = block * groups + group
    row0 = block * stride

    def scalar(name, i=0):
        return table_ref[row0 + (where[name] + i)]

    place = {"gx": (block, blocks), "yz": (group, groups)}

    def there(axis, shift):
        index, number = place[axis]
        return index + shift < number if shift > 0 else index + shift >= 0

    def other(axis, shift):
        index, number = place[axis]
        return {axis: jnp.clip(index + shift, 0, number - 1)}

    def partner(k):
        index = lax.rem(me + k, count)
        return {"gx": lax.div(index, groups), "yz": lax.rem(index, groups)}, index

    loads = []
    for slot, f in enumerate(PADDED):
        source = flow_ref if f == 4 else state_ref.at[f]
        for h in range(halves):
            loads.append(pltpu.make_async_copy(
                source.at[:, :, h * LANES:(h + 1) * LANES],
                pad.at[slot, h, :, TILE:TILE + width, :], load_sem.at[len(loads)],
            ))
    for slot, f in enumerate(PLAIN):
        loads.append(pltpu.make_async_copy(state_ref.at[f], plain.at[slot], load_sem.at[len(loads)]))
    spare = [
        pltpu.make_async_copy(source, target, load_sem.at[len(loads) + k])
        for k, (source, target) in enumerate((
            (cells_in, cells_ref), (table_in, table_ref), (cell_in, cell_ref), (zhi_in, zhi_ref), (zlo_in, zlo_ref),
            (normal_in, normal_ref), (pos_in, pos_ref), (observer_in, observer_ref), (bin_in, bin_ref),
        ))
    ]
    for load in spare[:2] + loads + spare[2:]:
        load.start()

    barrier = pltpu.get_barrier_semaphore()
    for k in range(1, count):
        pl.semaphore_signal(barrier, inc=1, device_id=partner(k)[0], device_id_type=MESH)

    for axis, shift, targets in (
        ("gx", -1, (left_sum, left_plane, asked.at[0], got.at[0])),
        ("gx", 1, (right_sum, right_plane, asked.at[1], got.at[1])),
        ("gx", -2, (far_left,)), ("gx", 2, (far_right,)),
    ):
        @pl.when(jnp.logical_not(there(axis, shift)))
        def _():
            for target in targets:
                target[...] = jnp.zeros_like(target)
    for shift, at in ((-1, TILE - REACH), (1, TILE + width)):
        @pl.when(jnp.logical_not(there("yz", shift)))
        def _():
            pad[:, :, :, at:at + REACH, :] = jnp.zeros((len(PADDED), halves, cells, REACH, LANES), jnp.float32)

    def remote(source, target, send, recv, axis, shift):
        return pltpu.make_async_remote_copy(
            src_ref=source, dst_ref=target, send_sem=send, recv_sem=recv,
            device_id=other(axis, shift), device_id_type=MESH,
        )

    def start(copy, axis, shift):
        @pl.when(there(axis, shift))
        def _():
            copy.start()

    def arrive(copy, axis, shift):
        @pl.when(there(axis, -shift))
        def _():
            copy.wait_recv()

    def sent(copy, axis, shift):
        @pl.when(there(axis, shift))
        def _():
            copy.wait_send()

    def near(side, t):
        if side == 0:
            return remote(on_right.at[t], left_sum.at[t], sum_send.at[0, t], sum_recv.at[0, t], "gx", 1), "gx", 1
        return remote(on_left.at[t], right_sum.at[t], sum_send.at[1, t], sum_recv.at[1, t], "gx", -1), "gx", -1

    def far(side, t):
        if side == 0:
            return remote(to_right.at[t], far_left.at[t], sum_send.at[2, t], sum_recv.at[2, t], "gx", 2), "gx", 2
        return remote(to_left.at[t], far_right.at[t], sum_send.at[3, t], sum_recv.at[3, t], "gx", -2), "gx", -2

    halos = [
        (remote(pad.at[:, :, :, TILE + width - REACH:TILE + width, :], pad.at[:, :, :, TILE - REACH:TILE, :],
                halo_send.at[0], halo_recv.at[0], "yz", 1), "yz", 1),
        (remote(pad.at[:, :, :, TILE:TILE + REACH, :], pad.at[:, :, :, TILE + width:TILE + width + REACH, :],
                halo_send.at[1], halo_recv.at[1], "yz", -1), "yz", -1),
    ]
    straight = lax.rem(block, 2)
    planes = [[], []]
    for side, (at, target, shift) in enumerate(((cells - 1, left_plane, 1), (0, right_plane, -1))):
        for piece, (source, into) in enumerate((
            (state_ref.at[0:2, at], target.at[0:2]), (state_ref.at[2:4, at], target.at[2:4]),
            (flow_ref.at[at], target.at[4]),
        )):
            planes[0 if piece in EARLY else 1].append((side, remote(
                source, into, plane_send.at[side, piece], plane_recv.at[side, piece], "gx", shift
            ), "gx", shift))

    def value(f, i, rows, h):
        if f in PADDED:
            return pad[PADDED.index(f), h, i, pl.ds(rows + TILE, TILE), :]
        return plain[PLAIN.index(f), i, pl.ds(rows, TILE), h * LANES:(h + 1) * LANES]

    def first_row(t):
        return pl.multiple_of(t * TILE, TILE)

    factor, shift = quotient(cells * width * groups, width * groups)
    power = depth.bit_length() - 1
    origin = block * (cells * width * groups)

    def locate(cell):
        line = (cell >> power if depth & (depth - 1) == 0 else lax.div(cell, depth)) - origin
        along_x = (line * factor) >> shift
        return along_x, line - along_x * (width * groups) - group * width

    spare[0].wait()
    ask[...] = jnp.full_like(ask, -1.0)
    along_x, along_y = locate(cells_ref[...])
    along_z = cells_ref[...] & (depth - 1) if depth & (depth - 1) == 0 else lax.rem(cells_ref[...], depth)
    for k, along in enumerate((along_y, along_z, along_x)):
        ask[k:k + 1, 0:faces] = along.astype(jnp.float32)
    asks = [
        (remote(ask, asked.at[0], ask_send.at[0], ask_recv.at[0], "gx", 1), "gx", 1),
        (remote(ask, asked.at[1], ask_send.at[1], ask_recv.at[1], "gx", -1), "gx", -1),
    ]
    replies = [
        (remote(reply.at[0], got.at[1], reply_send.at[0], reply_recv.at[0], "gx", -1), "gx", -1),
        (remote(reply.at[1], got.at[0], reply_send.at[1], reply_recv.at[1], "gx", 1), "gx", 1),
    ]

    pl.semaphore_wait(barrier, count - 1)
    for entry in asks:
        start(*entry)
    for side, *entry in planes[0]:
        @pl.when(straight == side)
        def _():
            start(*entry)
    for load in loads[:len(PADDED) * halves]:
        load.wait()
    for entry in halos:
        start(*entry)
    for load in loads[len(PADDED) * halves:] + spare[1:2]:
        load.wait()

    fields = range(5)
    pairs = [(f, h) for f in fields for h in range(halves)]

    def sums(t, carry):
        rows = first_row(t)
        totals = None
        for i in range(cells):
            weights = scalar("right", i), scalar("left", i)
            now = [value(f, i, rows, h) for f, h in pairs]
            terms = [[weight * one for weight in weights] for one in now]
            totals = terms if totals is None else [
                [old + new for old, new in zip(*both)] for both in zip(totals, terms)
            ]
        for (f, h), (total_right, total_left) in zip(pairs, totals):
            lanes = slice(h * LANES, (h + 1) * LANES)
            to_right[t, f, :, lanes] = total_right
            to_left[t, f, :, lanes] = total_left
        start(*far(0, t))
        start(*far(1, t))
        return carry

    lax.fori_loop(0, tiles, sums, 0)

    def relay(t):
        arrive(*far(0, t))
        arrive(*far(1, t))
        on_right[t] = to_right[t] + scalar("link", 0) * far_left[t]
        on_left[t] = to_left[t] + scalar("link", 1) * far_right[t]
        start(*near(0, t))
        start(*near(1, t))


    for load in spare[2:]:
        load.wait()

    together = 4 if cells % 4 == 0 else 1

    def multiply(k, carry):
        span = pl.ds(k * together, together)
        for f, target in ((0, 3), (3, 0), (4, 1)):
            if f in PADDED:
                lines = jnp.concatenate([
                    pad[PADDED.index(f), h, span, TILE:TILE + width, :].reshape(together * width, LANES)
                    for h in range(halves)
                ], axis=1)
            else:
                lines = plain[PLAIN.index(f), span].reshape(together * width, depth)
            high = lines.astype(jnp.bfloat16)
            rest = (lines - high.astype(jnp.float32)).astype(jnp.bfloat16)
            out = jnp.dot(rest, zhi_ref[...], preferred_element_type=jnp.float32)
            out += jnp.dot(high, zlo_ref[...], preferred_element_type=jnp.float32)
            out += jnp.dot(high, zhi_ref[...], preferred_element_type=jnp.float32)
            base[target, span] = out.reshape(together, width, depth)
        return carry

    steps = cells // together
    lax.fori_loop(0, steps // 2, multiply, 0)
    relay(0)
    lax.fori_loop(steps // 2, steps, multiply, 0)

    for entry in halos:
        arrive(*entry)

    def lateral(i, carry):
        for t in range(tiles):
            rows = t * TILE
            for h in range(halves):
                lanes = slice(h * LANES, (h + 1) * LANES)

                def y_rate(slot):
                    def take(shift):
                        return pad[slot, h, i, TILE + rows + shift:2 * TILE + rows + shift, :]
                    return (
                        0.75 * (take(1) - take(-1)) - 0.15 * (take(2) - take(-2))
                        + 1.0 / 60.0 * (take(3) - take(-3))
                    )

                spot = (i, slice(rows, rows + TILE), lanes)
                base[(0,) + spot] = base[(0,) + spot] + y_rate(1)
                base[(1,) + spot] = value(2, i, rows, h) * y_rate(2) + value(3, i, rows, h) * base[(1,) + spot]
                base[(2,) + spot] = y_rate(0)
        return carry

    pumps = max(tiles - 1, 1)
    for t in range(pumps):
        if t + 1 < tiles:
            relay(t + 1)
        lax.fori_loop(cells * t // pumps, cells * (t + 1) // pumps, lateral, 0)

    def plane_of(f, i):
        if f in PADDED:
            return jnp.concatenate(
                [pad[PADDED.index(f), h, i, TILE:TILE + width, :] for h in range(halves)], axis=1
            )
        return plain[PLAIN.index(f), i]

    def gather_columns(values, places):
        ahead = lax.broadcasted_iota(jnp.int32, (depth, places.shape[1]), 0).astype(jnp.float32)
        hot = jnp.where(ahead == places[1:2, :], 1.0, 0.0).astype(jnp.bfloat16)
        rest, total = jnp.concatenate(values, axis=0), None
        for _ in range(3):
            part = rest.astype(jnp.bfloat16)
            rest = rest - part.astype(jnp.float32)
            product = jnp.dot(part, hot, preferred_element_type=jnp.float32)
            total = product if total is None else total + product
        here = lax.broadcasted_iota(jnp.int32, (width, places.shape[1]), 0).astype(jnp.float32) == places[0:1, :]
        return [
            jnp.sum(jnp.where(here, total[k * width:(k + 1) * width], 0.0), axis=0, keepdims=True)
            for k in range(len(values))
        ]

    reply[...] = jnp.zeros_like(reply)
    for side, at in ((0, 0), (1, cells - 1)):
        arrive(*asks[side])
        for k, row in enumerate(gather_columns([plane_of(f, at) for f in fields], asked[side])):
            reply[side, k:k + 1, :] = row
        start(*replies[side])
    own = gather_columns([plane_of(f, at) for at in (0, cells - 1) for f in (1, 4)], ask[...])

    def find(k, carry):
        along_x, along_y = locate(cell_ref[k])
        along_x, along_y = jnp.clip(along_x, 0, cells - 1), jnp.clip(along_y, 0, width - 1)
        lines[k] = along_x * width + along_y
        for h in range(halves):
            chosen[h, pl.ds(k, 1), :] = pad[0, h, along_x, pl.ds(TILE + along_y, 1), :]
        return carry

    lax.fori_loop(0, faces, find, 0, unroll=4)

    geometry[...] = jnp.zeros_like(geometry)
    geometry[0:3, 0:faces] = normal_ref[...]
    geometry[3:6, 0:faces] = pos_ref[...]
    geometry[6:7, 0:faces] = along_z.astype(jnp.float32)
    columns_ref[...] = geometry[...].T

    def column(c):
        return columns_ref[0:faces, c:c + 1]

    normal = [column(c) for c in range(3)]
    offset = [observer_ref[c:c + 1, :] - column(3 + c) for c in range(3)]
    distance = jnp.sqrt(offset[0] * offset[0] + offset[1] * offset[1] + offset[2] * offset[2])
    normal_r = (normal[0] * offset[0] + normal[1] * offset[1] + normal[2] * offset[2]) / distance
    scale = 1.0 / (four_pi * distance)
    kernels[0] = scale
    kernels[1] = normal_r * scale
    kernels[2] = normal_r * scale / distance
    mask = lax.broadcasted_iota(jnp.int32, (faces, depth), 1) == column(6).astype(jnp.int32)
    nearby = jnp.concatenate([chosen[h] for h in range(halves)], axis=1)
    columns_ref[0:faces, 7:8] = jnp.sum(jnp.where(mask, nearby, 0.0), axis=1, keepdims=True)
    own_ref[...] = jnp.zeros_like(own_ref)
    for k, row in enumerate(own):
        own_ref[k:k + 1, :] = row

    chunk = 4
    assert cells % chunk == 0 and cells >= 3 * chunk

    def finish(t):
        rows = first_row(t)
        n = cells
        carry = []
        edge = [scalar("edge", j) for j in range(8)]
        link, end, back = scalar("link", 2), scalar("ends", 0), scalar("back", 1)
        for f, h in pairs:
            lanes = slice(h * LANES, (h + 1) * LANES)
            own = [value(f, i, rows, h) for i in range(4)]
            incoming = left_sum[t, f, :, lanes] + link * far_left[t, f, :, lanes]
            first = edge[0] * own[0] + edge[1] * own[1] + edge[2] * own[2] + end * incoming
            second = edge[4] * own[0] + edge[5] * own[1] + edge[6] * own[2] + edge[7] * own[3] - back * first
            swept[f, 0, :, lanes] = first
            swept[f, 1, :, lanes] = second
            carry.append(second)

        def forward(k, carry):
            i0 = 2 + k * chunk
            new = list(carry)
            factors = [[scalar(name, i0 + j) for name in ("near", "wide", "back")] for j in range(chunk)]
            for p, (f, h) in enumerate(pairs):
                lanes = slice(h * LANES, (h + 1) * LANES)
                own = [value(f, i0 + j, rows, h) for j in range(-2, chunk + 2)]
                for j in range(chunk):
                    close, wide, back = factors[j]
                    new[p] = close * (own[j + 3] - own[j + 1]) + wide * (own[j + 4] - own[j]) - back * new[p]
                    swept[f, i0 + j, :, lanes] = new[p]
            return tuple(new)

        carry = lax.fori_loop(0, (n - 4) // chunk, forward, tuple(carry))
        solved = []
        edge = [scalar("edge", 8 + j) for j in range(8)]
        link, end, back, last = scalar("link", 3), scalar("ends", 1), scalar("back", n - 2), scalar("back", n - 1)
        for p, (f, h) in enumerate(pairs):
            lanes = slice(h * LANES, (h + 1) * LANES)
            own = [value(f, i, rows, h) for i in range(n - 4, n)]
            incoming = right_sum[t, f, :, lanes] + link * far_right[t, f, :, lanes]
            before = (
                edge[0] * own[0] + edge[1] * own[1] + edge[2] * own[2] + edge[3] * own[3] - back * carry[p]
            )
            swept[f, n - 2, :, lanes] = before
            solved.append(
                edge[5] * own[1] + edge[6] * own[2] + edge[7] * own[3] + end * incoming - last * before
            )

        def store(i, x):
            spot = pl.ds(pl.multiple_of(i * width + rows, TILE), TILE)
            for h in range(halves):
                lanes = slice(h * LANES, (h + 1) * LANES)
                old = [value(f, i, rows, h) for f in fields]
                flow = old[4]
                px, ux, vx, wx, fx = (x[f * halves + h] for f in fields)
                terms = [base[c, i, pl.ds(rows, TILE), lanes] for c in range(4)]
                losses = (
                    flow * px + ux + terms[0],
                    flow * ux + old[1] * fx + px + terms[1],
                    flow * vx + terms[2],
                    flow * wx + terms[3],
                )
                for c in range(4):
                    rate[c, spot, lanes] = losses[c]
                    next_ref[c, i, pl.ds(rows, TILE), lanes] = old[c] - time_step * losses[c]

        def step_back(i, x):
            ahead = scalar("ahead", i)
            x = [
                swept[f, i, :, h * LANES:(h + 1) * LANES] - ahead * x[p]
                for p, (f, h) in enumerate(pairs)
            ]
            store(i, x)
            return x

        store(n - 1, solved)
        for j in range(2, chunk + 1):
            solved = step_back(n - j, solved)

        def backward(k, x):
            for j in range(chunk):
                x = step_back(n - chunk - 1 - k * chunk - j, x)
            return tuple(x)

        lax.fori_loop(0, n // chunk - 1, backward, tuple(solved))

    def main(t, carry):
        arrive(*near(0, t))
        arrive(*near(1, t))

        @pl.when(t == tiles - 1)
        def _():
            for side, *entry in planes[0]:
                @pl.when(straight != side)
                def _():
                    start(*entry)
            for side, *entry in planes[1]:
                start(*entry)

        finish(t)
        return carry

    lax.fori_loop(0, tiles, main, 0)

    for entry in replies:
        arrive(*entry)
    along = ask[2:3, :]
    first, last = along == 0.0, along == float(cells - 1)
    more = [
        jnp.where(first, scalar("ends", 2) * got[0, f:f + 1, :], 0.0)
        + jnp.where(last, scalar("ends", 3) * got[1, f:f + 1, :], 0.0) for f in fields
    ]
    stream, flow = (jnp.where(first, own_ref[k:k + 1, :], own_ref[2 + k:3 + k, :]) for k in range(2))
    mends[...] = jnp.zeros_like(mends)
    for c, row in enumerate((
        flow * more[0] + more[1], flow * more[1] + stream * more[4] + more[0], flow * more[2], flow * more[3],
    )):
        mends[c:c + 1, :] = row
    mended = mends[...].T

    def pick(k, carry):
        row = lines[k]
        for c in range(4):
            picked[c, pl.ds(k, 1), :] = rate[c, pl.ds(row, 1), :]
        return carry

    lax.fori_loop(0, faces, pick, 0, unroll=4)
    mask = lax.broadcasted_iota(jnp.int32, (faces, depth), 1) == column(6).astype(jnp.int32)
    at = [
        jnp.sum(jnp.where(mask, picked[c], 0.0), axis=1, keepdims=True) + mended[0:faces, c:c + 1] for c in range(4)
    ]
    pressure = column(7) - time_step * at[0]
    normal_rate = column(0) * at[1] + column(1) * at[2] + column(2) * at[3]
    contribution[...] = pressure * kernels[2] - at[0] * kernels[1] - normal_rate * kernels[0]

    def gather(k, carry):
        b0 = pl.multiple_of(k * TILE, TILE)
        for o in range(observers // LANES):
            lanes = slice(o * LANES, (o + 1) * LANES)
            totals = [jnp.zeros((TILE, LANES), jnp.float32)] * TILE
            for r in range(0, faces, TILE):
                bins, parts = bin_ref[r:r + TILE, lanes], contribution[r:r + TILE, lanes]
                totals = [
                    total + jnp.where(bins == b0 + j, parts, 0.0) for j, total in enumerate(totals)
                ]
            binned[pl.ds(b0, TILE), lanes] = jnp.concatenate(
                [jnp.sum(total, axis=0, keepdims=True) for total in totals], axis=0
            )
        return carry

    lax.fori_loop(0, BINS // TILE, gather, 0)
    share, beside = observers // count, LANES // BINS
    dense = share % (TILE * beside) == 0
    if not dense:
        pieces[...] = jnp.zeros_like(pieces)
    turned = jnp.concatenate([binned[...], jnp.zeros((LANES - BINS, observers), jnp.float32)], axis=0).T
    if dense:
        turned = turned.reshape(count, share // TILE, TILE, LANES)
        lane = lax.broadcasted_iota(jnp.int32, (count * TILE, LANES), 1)
        for q in range(share // TILE // beside):
            row = turned[:, q * beside].reshape(count * TILE, LANES)
            for j in range(1, beside):
                moved = pltpu.roll(turned[:, q * beside + j].reshape(count * TILE, LANES), j * BINS, 1)
                row = jnp.where(lane >= j * BINS, moved, row)
            pieces[:, q] = row.reshape(count, TILE, LANES)
    else:
        for d in range(count):
            pieces[d, 0, 0:share, :] = turned[d * share:(d + 1) * share]
    copies = []
    for k in range(1, count):
        target, index = partner(k)
        copies.append(pltpu.make_async_remote_copy(
            src_ref=pieces.at[index], dst_ref=landing.at[k - 1],
            send_sem=piece_send.at[k - 1], recv_sem=piece_recv.at[k - 1],
            device_id=target, device_id_type=MESH,
        ))
        copies[-1].start()
    for side, *entry in planes[0] + planes[1]:
        arrive(*entry)

    def mend(t, carry):
        rows = first_row(t)
        for at, plane, end in ((0, left_plane, 2), (cells - 1, right_plane, 3)):
            spot = pl.ds(pl.multiple_of(at * width + rows, TILE), TILE)
            for h in range(halves):
                lanes = slice(h * LANES, (h + 1) * LANES)
                px, ux, vx, wx, fx = (scalar("ends", end) * plane[f, pl.ds(rows, TILE), lanes] for f in fields)
                stream, flow = value(1, at, rows, h), value(4, at, rows, h)
                more = (flow * px + ux, flow * ux + stream * fx + px, flow * vx, flow * wx)
                for c in range(4):
                    rate[c, spot, lanes] = rate[c, spot, lanes] + more[c]
                    next_ref[c, at, pl.ds(rows, TILE), lanes] = (
                        next_ref[c, at, pl.ds(rows, TILE), lanes] - time_step * more[c]
                    )
        return carry

    lax.fori_loop(0, tiles, mend, 0)

    total = pieces[me]
    for k in range(count - 1):
        copies[k].wait_recv()
        total += landing[k]
    if dense:
        for q in range(share // TILE // beside):
            for j in range(beside):
                moved = total[q] if j == 0 else pltpu.roll(total[q], LANES - j * BINS, 1)
                top = (q * beside + j) * TILE
                signal_ref[top:top + TILE, :] = moved[:, 0:BINS]
    else:
        signal_ref[...] = total[0, 0:share, 0:BINS]

    for k in range(count - 1):
        copies[k].wait_send()
    for entry in halos + [tuple(entry) for side, *entry in planes[0] + planes[1]] + asks + replies:
        sent(*entry)

    def drain(t, carry):
        for side in (0, 1):
            sent(*near(side, t))
            sent(*far(side, t))
        return carry

    lax.fori_loop(0, tiles, drain, 0)


def copy_kernel(next_ref, signal_ref, next_out, signal_out, sems):
    copies = [
        pltpu.make_async_copy(next_ref, next_out, sems.at[0]),
        pltpu.make_async_copy(signal_ref, signal_out, sems.at[1]),
    ]
    for copy in copies:
        copy.start()
    for copy in copies:
        copy.wait()


def per_device(sizes, state, mean_flow, face_cell, face_normal, face_pos, observer_pos, time_bin):
    blocks, groups = sizes
    _, cells, width, depth = state.shape
    faces, observers = time_bin.shape
    tiles, halves, devices = width // TILE, depth // LANES, blocks * groups
    share = observers // devices
    dense = share % (TILE * (LANES // BINS)) == 0
    packed = (share * BINS // (TILE * LANES), TILE, LANES) if dense else (1, -(-share // TILE) * TILE, LANES)
    table = Table(blocks, cells)
    operator = dense_derivative(depth).T.astype(np.float32)
    z_high = jnp.asarray(operator).astype(jnp.bfloat16)
    z_low = (jnp.asarray(operator) - z_high.astype(jnp.float32)).astype(jnp.bfloat16)
    f32 = jnp.float32
    padded_faces = -(-faces // LANES) * LANES
    smem, vmem, hbm = (pl.BlockSpec(memory_space=space) for space in (SMEM, VMEM, HBM))
    dma = pltpu.SemaphoreType.DMA
    sums = VMEM((tiles, 5, TILE, depth), f32)
    state_next, signal = pl.pallas_call(
        functools.partial(fused_kernel, sizes, table.at, table.stride),
        out_shape=(VMEM(state.shape, f32), VMEM((share, BINS), f32)),
        in_specs=[hbm] * 11,
        out_specs=(vmem, vmem),
        scratch_shapes=[
            SMEM(table.values.shape, f32), SMEM((faces,), jnp.int32), VMEM((1, faces), jnp.int32),
            VMEM((3, faces), f32), VMEM((3, faces), f32), VMEM((3, observers), f32),
            VMEM((depth, depth), jnp.bfloat16), VMEM((depth, depth), jnp.bfloat16),
            VMEM((faces, observers), jnp.int32),
            VMEM((len(PADDED), halves, cells, width + 2 * TILE, LANES), f32),
            VMEM((len(PLAIN), cells, width, depth), f32),
            VMEM((4, cells, width, depth), f32),
            VMEM((5, cells, TILE, depth), f32),
            VMEM((4, cells * width, depth), f32),
        ] + [sums] * 8 + [
            VMEM((5, width, depth), f32), VMEM((5, width, depth), f32),
            VMEM((TILE, padded_faces), f32), VMEM((3, faces, observers), f32),
            VMEM((4, faces, depth), f32), VMEM((faces, observers), f32),
            VMEM((BINS, observers), f32), VMEM((devices,) + packed, f32),
            VMEM((devices - 1,) + packed, f32),
            SMEM((faces,), jnp.int32), VMEM((halves, faces, LANES), f32), VMEM((TILE, padded_faces), f32), VMEM((2, TILE, padded_faces), f32),
            VMEM((2, TILE, padded_faces), f32), VMEM((2, TILE, padded_faces), f32),
            VMEM((TILE, padded_faces), f32), VMEM((padded_faces, TILE), f32), VMEM((TILE, padded_faces), f32),
            dma((len(PADDED) * halves + len(PLAIN) + 9,)), dma((2,)), dma((2,)), dma((2, 3)), dma((2, 3)),
            dma((4, tiles)), dma((4, tiles)), dma((devices - 1,)), dma((devices - 1,)),
            dma((2,)), dma((2,)), dma((2,)), dma((2,)),
        ],
        compiler_params=pltpu.CompilerParams(
            collective_id=0, has_side_effects=True, vmem_limit_bytes=VMEM_MIB * 1024 * 1024
        ),
    )(
        jnp.asarray(table.values), face_cell, state, mean_flow, z_high, z_low,
        face_cell.reshape(1, faces), face_normal, face_pos, observer_pos, time_bin,
    )
    return pl.pallas_call(
        copy_kernel,
        out_shape=(
            jax.ShapeDtypeStruct(state.shape, f32),
            jax.ShapeDtypeStruct((share, BINS), f32),
        ),
        in_specs=[vmem, vmem],
        out_specs=(hbm, hbm),
        scratch_shapes=[dma((2,))],
        compiler_params=pltpu.CompilerParams(vmem_limit_bytes=8 * 1024 * 1024),
    )(state_next, signal)


def solution(mesh):
    in_specs = (
        P(None, "gx", "yz", None),
        P("gx", "yz", None),
        P(("gx", "yz")),
        P(None, ("gx", "yz")),
        P(None, ("gx", "yz")),
        P(),
        P(("gx", "yz"), None),
    )
    out_specs = (P(None, "gx", "yz", None), P(("gx", "yz"), None))
    sizes = (mesh.shape["gx"], mesh.shape["yz"])
    return jax.shard_map(
        functools.partial(per_device, sizes),
        mesh=mesh, in_specs=in_specs, out_specs=out_specs, check_vma=False,
    )
```
